128 devices in a mesh: grp: 4 (over x, y), tok: 16 (over z), mdl: 2 (over core).
Axes of the slice: x: 2, y: 2, z: 16, core: 2. Of those that a mesh axis runs over, the one named last changes fastest.
The devices are a block of a 8x8x16 slice.
Arguments:
- hidden: bfloat16 [4096, 4096], P(('grp', 'tok'), 'mdl'), parts along dimension 0, may hold values from -3 to 3
- queries: bfloat16 [4096, 16, 128], P(('grp', 'tok'), 'mdl'), parts along dimension 0, may hold values from -8 to 8
- cache: bfloat16 [64, 2048, 4, 2, 128], P(('grp', 'tok'), None, 'mdl'), parts along dimension 0, may hold values from -8 to 8
- cache_lengths: int32 [64], P(('grp', 'tok')), parts along dimension 0, may hold values from 128 to 2048, as said below
- wkv: bfloat16 [4096, 4, 2, 128], P('tok', 'mdl'), may hold values from -0.09375 to 0.09375
- wo: bfloat16 [16, 128, 4096], P('mdl', None, 'tok'), may hold values from -0.5 to 0.5
- attn_gain: bfloat16 [4096], replicated, may hold values from 0.5 to 1.5
- moe_gain: bfloat16 [4096], replicated, may hold values from 0.5 to 1.5
- w_gate: bfloat16 [32, 4096, 896], P(('tok', 'mdl')), may hold values from -0.09375 to 0.09375
- w_up: bfloat16 [32, 4096, 896], P(('tok', 'mdl')), may hold values from -0.09375 to 0.09375
- w_down: bfloat16 [32, 896, 4096], P(('tok', 'mdl')), may hold values from -0.0625 to 0.0625
- expert_ids: int32 [4096, 2], P(('grp', 'tok', 'mdl')), parts along dimension 0, may hold values from 0 to 3, all different within a row; in each aligned block of 32 rows (0 to 31, 32 to 63, ...) at most 18 rows name the same one
- gates: float32 [4096, 2], P(('grp', 'tok', 'mdl')), parts along dimension 0, may hold values from 0.1 to 1
Outputs:
- mixed: bfloat16 [4096, 4096], P(('grp', 'tok', 'mdl')), parts along dimension 0
- fresh_key_value: bfloat16 [4096, 4, 2, 128], P(('grp', 'tok'), 'mdl'), parts along dimension 0
The draws below stay inside these ranges and needn't reach their ends.
There are 4 independent parts, one for each index of `grp`. The reference program is written for one: setup_inputs(seed, part) draws one part's arguments, and reference() takes and returns one part's arrays. A program takes and returns all parts, laid end to end along the dimension named above; an argument that names none is the same for every part. Nothing has to cross between parts.
Inputs may be any that keep to these rules, and one draw needn't show every extreme that they name: `expert_ids`: each token names 2 different experts; in aligned blocks of 32 rows no expert is named by more than 18 rows, a bound that some block reaches. `cache_lengths`: some rollout holds exactly 2048 cached positions.
All inputs are finite; a program needn't handle non-finite values.
Results may differ from the reference program's by a relative error of at most 0.007.
Values may be sent and summed in bfloat16 or wider, within the bound.
A program may use at most 128 MiB of HBM per device.

```python
import math
import jax
import jax.numpy as jnp
import numpy as np
from jax import lax

MODEL_DIM = 4096
HEAD_SIZE = 128
QUERY_HEADS = 16
KEY_VALUE_HEADS = 4
EXPERTS = 4
FF = 7168
TOPK = 2
NEW_TOKEN_SPAN = 64
CACHE_LIMIT = 2048
ROLLOUT_COUNT = 16
TOKEN_TOTAL = 1024
TOK_MOE = 32
CAP = 18
SLABS = 8
FS = 896
N_TOK = 16
N_MDL = 2


def draw_queries(key, part):
    array_shape = (TOKEN_TOTAL, QUERY_HEADS, HEAD_SIZE)
    return jnp.clip(jax.random.normal(jax.random.fold_in(key, 1), array_shape, jnp.float32) * 2.5, -7.5, 7.5).astype(jnp.bfloat16)


def draw_cache(key, part):
    array_shape = (ROLLOUT_COUNT, CACHE_LIMIT, KEY_VALUE_HEADS, 2, HEAD_SIZE)
    return jnp.clip(jax.random.normal(jax.random.fold_in(key, 2), array_shape, jnp.float32), -5.0, 5.0).astype(jnp.bfloat16)


def draw_cache_lengths(key, part):
    values = jax.random.randint(jax.random.fold_in(key, 3), (ROLLOUT_COUNT,), CACHE_LIMIT // 16, CACHE_LIMIT + 1)
    longest = jax.random.randint(jax.random.fold_in(key, 4), (), 0, ROLLOUT_COUNT)
    return jnp.where(jnp.arange(ROLLOUT_COUNT) == longest, CACHE_LIMIT, values).astype(jnp.int32)


def block_scale(stream_key, dims, split, smallest, top_value):
    level = 1.0
    for position, shards_of in split:
        steps = jax.random.uniform(jax.random.fold_in(jax.random.fold_in(stream_key, 6), position), (shards_of,), jnp.float32, smallest / len(split), top_value / len(split))
        level = level * jnp.repeat(jnp.exp(steps), dims[position] // shards_of).reshape((-1,) + (1,) * (len(dims) - 1 - position))
    return level


def routed_block(stream_key, own, number, rows, count, top, most, slope):
    ranking = jax.random.permutation(stream_key, count)
    crowded, usual = load_shares(count, rows * top, most, slope, True), load_shares(count, rows * top, most, slope, False)
    places = jnp.arange(count)

    def named(tallies, rotation):
        used = int((tallies > 0).sum())
        fixed = max(1, used // 4)
        shifted = fixed + (places - fixed + rotation * (used - fixed)) % max(1, count - fixed)
        return jnp.zeros((count,), jnp.int32).at[ranking[jnp.where(places < fixed, places, shifted)]].set(jnp.asarray(tallies, jnp.int32))

    tallies = jnp.where(number % 4 == 0, named(crowded, number // 4), named(usual, number - number // 4 - 1))
    mixed = jax.random.permutation(jax.random.fold_in(own, 3), count)
    source_of, receiver = mixed[0:count // 2 * 2:2], mixed[1:count // 2 * 2:2]
    room = jnp.minimum(tallies[source_of] - 1, most - tallies[receiver]) // 2
    room = jnp.where((source_of == ranking[0]) | (receiver == ranking[0]) | (tallies[receiver] == 0), 0, jnp.maximum(room, 0))
    shifted = jax.random.randint(jax.random.fold_in(own, 4), (count // 2,), 0, 1 << 20) % (room + 1)
    tallies = tallies.at[source_of].add(-shifted).at[receiver].add(shifted)
    items = jnp.searchsorted(jnp.cumsum(tallies), jnp.arange(rows * top), side="right").astype(jnp.int32)
    grid = items.reshape(top, rows).T
    grid = grid[jax.random.permutation(jax.random.fold_in(own, 1), rows)]
    rotation = jax.random.randint(jax.random.fold_in(own, 2), (rows, 1), 0, top)
    return jnp.take_along_axis(grid, (jnp.arange(top)[None, :] + rotation) % top, axis=1)


def load_shares(amount, total, reach, skew, full):
    weights = [(1 << 20) // math.isqrt(rank ** skew) + 1 for rank in range(1, amount + 1)]
    largest = reach if full else min(reach, max(-(-total // amount), total * weights[0] // sum(weights)))
    least = 1 if total - largest >= amount - 1 else 0
    holding, surplus = [largest] + [least] * (amount - 1), total - largest - least * (amount - 1)
    while surplus > 0:
        candidates = [i for i in range(1, amount) if holding[i] < largest] or [i for i in range(1, amount) if holding[i] < reach]
        whole, left = sum([weights[i] for i in candidates]), surplus
        for i in candidates:
            extra = min(reach - holding[i], max(1, left * weights[i] // whole), surplus)
            holding[i] = holding[i] + extra
            surplus = surplus - extra
    return np.array(holding)


def bell_draw(rng, shape, width, most, split=(), kind=jnp.bfloat16):
    drawn = width * jax.random.normal(rng, shape, jnp.float32)
    if split:
        drawn = drawn * block_scale(rng, shape, split, -0.22, 0.18)
    return jnp.clip(drawn, -most, most).astype(kind)


def setup_inputs(seed: int = 0, part: int = 0) -> dict:
    key_of = jax.random.split(jax.random.key(seed), 14)
    part_keys = jax.random.split(jax.random.fold_in(key_of[13], part), 14)
    hidden = bell_draw(part_keys[0], (TOKEN_TOTAL, MODEL_DIM), 0.5, 3.0, ((0, 16), (1, 2)))
    queries = draw_queries(jax.random.fold_in(jax.random.fold_in(key_of[13], part), 71), part)
    cache = draw_cache(jax.random.fold_in(jax.random.fold_in(key_of[13], part), 71), part)
    cache_lengths = draw_cache_lengths(jax.random.fold_in(jax.random.fold_in(key_of[13], part), 71), part)
    wkv = bell_draw(key_of[4], (MODEL_DIM, KEY_VALUE_HEADS, 2, HEAD_SIZE), MODEL_DIM ** -0.5, 0.09375, ((0, 16), (1, 2)))
    wo = bell_draw(key_of[5], (QUERY_HEADS, HEAD_SIZE, MODEL_DIM), HEAD_SIZE ** -0.5, 0.5, ((0, 2), (2, 16)))
    attn_gain = jnp.clip(1.0 + 0.1 * jax.random.normal(key_of[6], (MODEL_DIM,), jnp.float32), 0.5, 1.5).astype(jnp.bfloat16)
    moe_gain = jnp.clip(1.0 + 0.1 * jax.random.normal(key_of[7], (MODEL_DIM,), jnp.float32), 0.5, 1.5).astype(jnp.bfloat16)
    w_gate = bell_draw(key_of[8], (EXPERTS * SLABS, MODEL_DIM, FS), MODEL_DIM ** -0.5, 0.09375, ((0, 32),))
    w_up = bell_draw(key_of[9], (EXPERTS * SLABS, MODEL_DIM, FS), MODEL_DIM ** -0.5, 0.09375, ((0, 32),))
    w_down = bell_draw(key_of[10], (EXPERTS * SLABS, FS, MODEL_DIM), FF ** -0.5, 0.0625, ((0, 32),))
    expert_ids_keys = jax.random.split(jax.random.fold_in(part_keys[11], 1), TOKEN_TOTAL // TOK_MOE)
    expert_ids_turns = jax.random.permutation(jax.random.fold_in(part_keys[11], 3), TOKEN_TOTAL // TOK_MOE)
    expert_ids = jax.vmap(lambda own, number: routed_block(jax.random.fold_in(part_keys[11], 2), own, number, TOK_MOE, EXPERTS, TOPK, CAP, 2))(expert_ids_keys, expert_ids_turns).reshape((TOKEN_TOTAL, TOPK))
    gates = jnp.clip(0.1 + 0.9 * jax.random.uniform(part_keys[12], (TOKEN_TOTAL, TOPK), jnp.float32) ** block_scale(part_keys[12], (TOKEN_TOTAL, TOPK), ((0, 32),), -0.2, 0.2), 0.1, 1.0)
    return dict(hidden=hidden, queries=queries, cache=cache, cache_lengths=cache_lengths, wkv=wkv, wo=wo, attn_gain=attn_gain, moe_gain=moe_gain, w_gate=w_gate, w_up=w_up, w_down=w_down, expert_ids=expert_ids, gates=gates)


eps_norm = 1e-05
rope_base = 1000000.0
mask_fill = -1e+30

def rms_scale(values_in, gain):
    values = values_in.astype(jnp.float32)
    meansq = lax.optimization_barrier(jnp.mean(values * values, axis=-1, keepdims=True))
    return values * lax.rsqrt(meansq + eps_norm) * gain.astype(jnp.float32)

def rotate(key_rows, positions):
    half_dim = key_rows.shape[-1] // 2
    inverse = jnp.exp(jnp.arange(half_dim, dtype=jnp.float32) * (-2.0 * math.log(rope_base) / key_rows.shape[-1]))
    angle = positions.astype(jnp.float32)[:, None] * inverse[None, :]
    cosine = jnp.cos(angle)[:, None, :]
    sine_vals = jnp.sin(angle)[:, None, :]
    front_half = key_rows[..., :half_dim]
    back_half = key_rows[..., half_dim:]
    return jnp.concatenate([front_half * cosine - back_half * sine_vals, back_half * cosine + front_half * sine_vals], axis=-1)

def reference(hidden, queries, cache, cache_lengths, wkv, wo, attn_gain, moe_gain, w_gate, w_up, w_down, expert_ids, gates):
    normalized_input = rms_scale(hidden, attn_gain).astype(jnp.bfloat16)
    key_value_projection = jnp.dot(normalized_input, wkv.reshape(MODEL_DIM, KEY_VALUE_HEADS * 2 * HEAD_SIZE), preferred_element_type=jnp.float32).reshape(TOKEN_TOTAL, KEY_VALUE_HEADS, 2, HEAD_SIZE)
    positions = (cache_lengths[:, None] + jnp.arange(NEW_TOKEN_SPAN, dtype=jnp.int32)[None, :]).reshape(TOKEN_TOTAL).astype(jnp.int32)
    fresh_key_value = jnp.stack([rotate(key_value_projection[:, :, 0], positions), key_value_projection[:, :, 1]], axis=2).astype(jnp.bfloat16)
    head_group = QUERY_HEADS // KEY_VALUE_HEADS
    scale_factor = 1.0 / math.sqrt(HEAD_SIZE)
    query_all = queries.reshape(ROLLOUT_COUNT, NEW_TOKEN_SPAN, QUERY_HEADS, HEAD_SIZE)
    fresh_all_rows = fresh_key_value.reshape(ROLLOUT_COUNT, NEW_TOKEN_SPAN, KEY_VALUE_HEADS, 2, HEAD_SIZE)

    def one_rollout(packed):
        query_roll, cache_roll, new_roll, length = packed
        token_of_row = jnp.arange(NEW_TOKEN_SPAN * head_group) // head_group
        column = jnp.arange(CACHE_LIMIT + NEW_TOKEN_SPAN)
        allowed = jnp.where(column[None, :] < CACHE_LIMIT, column[None, :] < length, column[None, :] - CACHE_LIMIT <= token_of_row[:, None])
        outputs = []
        for head_index in range(KEY_VALUE_HEADS):
            query_rows = query_roll[:, head_index * head_group:(head_index + 1) * head_group].reshape(NEW_TOKEN_SPAN * head_group, HEAD_SIZE)
            key_rows = jnp.concatenate([cache_roll[:, head_index, 0], new_roll[:, head_index, 0]], axis=0)
            value_rows = jnp.concatenate([cache_roll[:, head_index, 1], new_roll[:, head_index, 1]], axis=0)
            scores = lax.dot_general(query_rows, key_rows, (((1,), (1,)), ((), ())), preferred_element_type=jnp.float32) * scale_factor
            scores = jnp.where(allowed, scores, mask_fill)
            row_max = lax.optimization_barrier(jnp.max(scores, axis=1, keepdims=True))
            weights = jnp.where(allowed, jnp.exp(scores - row_max), 0.0)
            probs = (weights / lax.optimization_barrier(jnp.sum(weights, axis=1, keepdims=True))).astype(jnp.bfloat16)
            attended = jnp.dot(probs, value_rows, preferred_element_type=jnp.float32).astype(jnp.bfloat16)
            outputs.append(attended.reshape(NEW_TOKEN_SPAN, head_group * HEAD_SIZE))
        return jnp.concatenate(outputs, axis=1)
    heads_out = lax.map(one_rollout, (query_all, cache, fresh_all_rows, cache_lengths)).reshape(TOKEN_TOTAL, QUERY_HEADS * HEAD_SIZE)
    attn_out = jnp.dot(heads_out, wo.reshape(QUERY_HEADS * HEAD_SIZE, MODEL_DIM), preferred_element_type=jnp.float32)
    resid = hidden.astype(jnp.float32) + attn_out
    moe_in = rms_scale(resid, moe_gain).astype(jnp.bfloat16)
    limit = N_TOK * N_MDL * CAP
    moe_out = jnp.zeros((TOKEN_TOTAL, MODEL_DIM), jnp.float32)
    for expert_idx in range(EXPERTS):
        match = expert_ids == expert_idx
        routed = jnp.any(match, axis=1)
        weight = lax.optimization_barrier(jnp.sum(jnp.where(match, gates, 0.0), axis=1)).astype(jnp.float32)
        order = jnp.argsort(jnp.where(routed, 0, 1).astype(jnp.int32), stable=True)[:limit].astype(jnp.int32)
        rows_in = moe_in[order]

        def slab_step(total, slab_idx):
            row_idx = expert_idx * SLABS + slab_idx
            gate_w = lax.dynamic_index_in_dim(w_gate, row_idx, 0, keepdims=False)
            up_w = lax.dynamic_index_in_dim(w_up, row_idx, 0, keepdims=False)
            down_w = lax.dynamic_index_in_dim(w_down, row_idx, 0, keepdims=False)
            gate_val = jnp.dot(rows_in, gate_w, preferred_element_type=jnp.float32)
            up_val = jnp.dot(rows_in, up_w, preferred_element_type=jnp.float32)
            slab_hidden = (jax.nn.silu(gate_val) * up_val).astype(jnp.bfloat16)
            slab_out = jnp.dot(slab_hidden, down_w, preferred_element_type=jnp.float32).astype(jnp.bfloat16)
            return (total + slab_out.astype(jnp.float32), None)
        total, unused = lax.scan(slab_step, jnp.zeros((limit, MODEL_DIM), jnp.float32), jnp.arange(SLABS, dtype=jnp.int32))
        moe_out = moe_out.at[order].add(weight[order][:, None] * total)
    mixed = (resid + moe_out).astype(jnp.bfloat16)
    return (mixed, fresh_key_value)
```

```python
import functools
import math

import jax
import jax.numpy as jnp
from jax import lax
from jax.experimental import pallas as pl
from jax.experimental.pallas import tpu as pltpu
from jax.sharding import PartitionSpec as P

EXPERTS = 4
TOPK = 2

eps_norm = 1e-05
rope_base = 1000000.0
mask_fill = -1e30

MESH = pl.DeviceIdType.MESH
bf16 = jnp.bfloat16
f32 = jnp.float32


def joined_along(tiles, dim):
    dims = list(tiles.shape[1:])
    dims[dim] *= tiles.shape[0]
    return jnp.moveaxis(tiles, 0, dim).reshape(dims)


def sent_to_all(shard, axis):
    copies = jnp.broadcast_to(shard, (lax.axis_size(axis), *shard.shape))
    return lax.all_to_all(copies, axis, split_axis=0, concat_axis=0, tiled=True)


def collect(shard, axis, dim):
    return joined_along(sent_to_all(shard, axis), dim)


def in_blocks(shard, dim, size):
    dims = shard.shape
    tiles = shard.reshape(*dims[:dim], size, dims[dim] // size, *dims[dim + 1 :])
    return jnp.moveaxis(tiles, dim, 0)


def sent_and_summed(shard, axis, dim):
    tiles = in_blocks(shard, dim, lax.axis_size(axis))
    arrived = lax.all_to_all(tiles, axis, split_axis=0, concat_axis=0, tiled=True)
    return arrived.sum(axis=0)


def rms_scale(values_in, gain):
    values = values_in.astype(jnp.float32)
    meansq = jnp.mean(values * values, axis=-1, keepdims=True)
    return values * lax.rsqrt(meansq + eps_norm) * gain.astype(jnp.float32)


def rotate(key_rows, positions):
    half_dim = key_rows.shape[-1] // 2
    inverse = jnp.exp(
        jnp.arange(half_dim, dtype=jnp.float32) * (-2.0 * math.log(rope_base) / key_rows.shape[-1])
    )
    angle = positions.astype(jnp.float32)[:, None] * inverse[None, :]
    cosine = jnp.cos(angle)[:, None, :]
    sine_vals = jnp.sin(angle)[:, None, :]
    front_half = key_rows[..., :half_dim]
    back_half = key_rows[..., half_dim:]
    return jnp.concatenate(
        [front_half * cosine - back_half * sine_vals, back_half * cosine + front_half * sine_vals],
        axis=-1,
    )


def score_rows(query_rows, key_rows, scale_factor):
    return (
        lax.dot_general(
            query_rows, key_rows, (((1,), (1,)), ((), ())), preferred_element_type=jnp.float32
        )
        * scale_factor
    )


def head_attention(query_rows, cache_keys, cache_values, length, new_keys, new_values, head_group):
    row_count = query_rows.shape[0]
    block_len = min(512, cache_keys.shape[0])
    scale_factor = 1.0 / math.sqrt(query_rows.shape[1])
    token_of_row = jnp.arange(row_count) // head_group
    block_total = (length + block_len - 1) // block_len

    def block_scores(block_idx):
        row_offset = block_idx * block_len
        block_keys = lax.dynamic_slice_in_dim(cache_keys, row_offset, block_len, 0)
        allowed = row_offset + jnp.arange(block_len) < length
        return (
            jnp.where(
                allowed[None, :], score_rows(query_rows, block_keys, scale_factor), mask_fill
            ),
            allowed,
        )

    new_allowed = jnp.arange(new_keys.shape[0])[None, :] <= token_of_row[:, None]
    new_scores = jnp.where(new_allowed, score_rows(query_rows, new_keys, scale_factor), mask_fill)
    first_max = jnp.max(new_scores, axis=1)
    first_sum = jnp.sum(
        jnp.where(new_allowed, jnp.exp(new_scores - first_max[:, None]), 0.0), axis=1
    )

    def first_pass(block_idx, carry):
        run_max, run_sum = carry
        scores, allowed = block_scores(block_idx)
        next_max = jnp.maximum(run_max, jnp.max(scores, axis=1))
        weights = jnp.where(allowed[None, :], jnp.exp(scores - next_max[:, None]), 0.0)
        return (next_max, run_sum * jnp.exp(run_max - next_max) + jnp.sum(weights, axis=1))

    row_max, row_sum = lax.fori_loop(0, block_total, first_pass, (first_max, first_sum))
    new_probs = (
        jnp.where(new_allowed, jnp.exp(new_scores - row_max[:, None]), 0.0) / row_sum[:, None]
    ).astype(jnp.bfloat16)
    start_total = jnp.dot(new_probs, new_values, preferred_element_type=jnp.float32)

    def second_pass(block_idx, total):
        scores, allowed = block_scores(block_idx)
        probs = (
            jnp.where(allowed[None, :], jnp.exp(scores - row_max[:, None]), 0.0) / row_sum[:, None]
        ).astype(jnp.bfloat16)
        block_values = lax.dynamic_slice_in_dim(cache_values, block_idx * block_len, block_len, 0)
        return total + jnp.dot(probs, block_values, preferred_element_type=jnp.float32)

    total = lax.fori_loop(0, block_total, second_pass, start_total)
    return total.astype(jnp.bfloat16)


LANES = 128
GT = 256
DT = 512


def expert_kernel(
    half,
    x_ref,
    resid_ref,
    wg_hbm,
    wu_hbm,
    wd_hbm,
    out_ref,
    xs,
    wgu,
    wd,
    gu,
    hid,
    mine,
    pout,
    pin,
    rsin,
    wsem,
    ag_send,
    ag_recv,
    x_send,
    x_recv,
    p_send,
    p_recv,
    rs_send,
    rs_recv,
):
    ring = 2 * half
    z = lax.axis_index("tok")
    m = lax.axis_index("mdl")
    ahead = lax.rem(z + 1, ring)
    behind = lax.rem(z + ring - 1, ring)
    partner = {"mdl": 1 - m}
    expert = z // (ring // EXPERTS)
    block, width = resid_ref.shape
    ffs = wg_hbm.shape[1]
    wide = x_ref.shape[1]
    cut = width // 2
    spans = ((0, cut), (cut, wide - cut))
    ospans = ((0, cut), (cut, width - cut))

    loads = (
        pltpu.make_async_copy(wg_hbm, wgu.at[:, pl.ds(0, ffs)], wsem.at[0]),
        pltpu.make_async_copy(wu_hbm, wgu.at[:, pl.ds(ffs, ffs)], wsem.at[1]),
        pltpu.make_async_copy(wd_hbm, wd, wsem.at[2]),
    )

    barrier = pltpu.get_barrier_semaphore()
    for who in ({"tok": ahead}, {"tok": behind}, partner):
        pl.semaphore_signal(barrier, inc=1, device_id=who, device_id_type=MESH)
    pl.semaphore_wait(barrier, 3)

    def ring_copy(src, dst_slot, flow, piece, step):
        lo, size = spans[piece]
        return pltpu.make_async_remote_copy(
            src_ref=src.at[:, pl.ds(lo, size)],
            dst_ref=xs.at[dst_slot, 0, :, pl.ds(lo, size)],
            send_sem=ag_send.at[step, flow, piece],
            recv_sem=ag_recv.at[step, flow, piece],
            device_id={"tok": behind if flow == 0 else ahead},
            device_id_type=MESH,
        )

    def partner_copy(src, slot, piece):
        lo, size = spans[piece]
        return pltpu.make_async_remote_copy(
            src_ref=src.at[:, pl.ds(lo, size)],
            dst_ref=xs.at[slot, 1, :, pl.ds(lo, size)],
            send_sem=x_send.at[slot, piece],
            recv_sem=x_recv.at[slot, piece],
            device_id=partner,
            device_id_type=MESH,
        )

    def first_slot(flow, piece):
        return 2 + flow if half > 1 else 1

    for piece in range(2):
        for flow in range(2):
            ring_copy(x_ref, 2 + flow, flow, piece, 1).start()
    for load in loads:
        load.start()
    for piece in range(2):
        partner_copy(x_ref, 0, piece).start()
    xs[0, 0] = x_ref[...]

    def gate_up(g, lo, hi):
        def tile(n, carry):
            cols = pl.ds(pl.multiple_of(n * GT, GT), GT)
            rows = xs[pl.ds(2 * g, 2), :, :, pl.ds(0, width)].reshape(4 * block, width)
            gu[:, cols] = jnp.dot(rows, wgu[:, cols], preferred_element_type=f32)
            return carry

        lax.fori_loop(lo, hi, tile, 0)

    def activate():
        gate = gu[:, pl.ds(0, ffs)]
        up = gu[:, pl.ds(ffs, ffs)]
        hid[...] = (gate / (1.0 + jnp.exp(-gate)) * up).astype(bf16)

    def weight_of(g):
        tail = xs[pl.ds(2 * g, 2), :, :, pl.ds(width, LANES)].reshape(4 * block, LANES)
        lane = lax.broadcasted_iota(jnp.int32, (4 * block, LANES), 1)
        pick = (lane == expert) | (lane == expert + EXPERTS)
        return jnp.sum(jnp.where(pick, tail.astype(f32), 0.0), axis=1, keepdims=True)

    def down(g, lo, hi):
        weight = weight_of(g)

        def tile(n, carry):
            cols = pl.ds(pl.multiple_of(n * DT, DT), DT)
            got = jnp.dot(hid[...], wd[:, cols], preferred_element_type=f32) * weight
            got = got.astype(bf16)
            for slot in range(2):
                mine[2 * g + slot, :, cols] = got[2 * slot * block : (2 * slot + 1) * block]
                pout[2 * g + slot, :, cols] = got[(2 * slot + 1) * block : (2 * slot + 2) * block]
            return carry

        lax.fori_loop(lo, hi, tile, 0)

    gtiles = 2 * ffs // GT
    dtiles = width // DT

    def give(g):
        return pltpu.make_async_remote_copy(
            src_ref=pout.at[pl.ds(2 * g, 2)],
            dst_ref=pin.at[pl.ds(2 * g, 2)],
            send_sem=p_send.at[g],
            recv_sem=p_recv.at[g],
            device_id=partner,
            device_id_type=MESH,
        )

    def await_partner(g):
        for slot in range(2):
            for piece in range(2):
                partner_copy(x_ref, 2 * g + slot, piece).wait_recv()

    def arrive(s, flow, piece, onward):
        ring_copy(x_ref, 2 * s + flow, flow, piece, s).wait_recv()
        if onward is not None:
            ring_copy(xs.at[2 * s + flow, 0], onward, flow, piece, s + 1).start()
        partner_copy(xs.at[2 * s + flow, 0], 2 * s + flow, piece).start()

    def first_part(g):
        await_partner(g)
        gate_up(g, 0, gtiles)

    def second_part(g):
        activate()
        down(g, 0, dtiles)
        give(g).start()

    for flow in range(2):
        arrive(1, flow, 0, 4 + flow)
    for load in loads:
        load.wait()
    for flow in range(2):
        arrive(1, flow, 1, 4 + flow)

    def body(s, carry):
        for flow in range(2):
            arrive(s, flow, 0, 2 * (s + 1) + flow)
        first_part(s - 1)
        for flow in range(2):
            arrive(s, flow, 1, 2 * (s + 1) + flow)
        second_part(s - 1)
        return carry

    lax.fori_loop(2, half - 1, body, 0)

    last = half - 1
    arrive(last, 0, 0, 1)
    arrive(last, 1, 0, None)
    first_part(last - 1)
    arrive(last, 0, 1, None)
    arrive(last, 1, 1, 1)
    second_part(last - 1)

    await_partner(last)
    gate_up(last, 0, gtiles)
    for flow in range(2):
        ring_copy(x_ref, 1, flow, flow, half).wait_recv()
        partner_copy(xs.at[1, 0], 1, flow).start()
    second_part(last)
    await_partner(0)
    gate_up(0, 0, gtiles)
    activate()
    down(0, 0, dtiles)
    give(0).start()

    def sum_copy(slot, flow, piece, step):
        lo, size = ospans[piece]
        return pltpu.make_async_remote_copy(
            src_ref=mine.at[slot, :, pl.ds(lo, size)],
            dst_ref=rsin.at[flow, step, :, pl.ds(lo, size)],
            send_sem=rs_send.at[step, flow, piece],
            recv_sem=rs_recv.at[step, flow, piece],
            device_id={"tok": ahead if flow == 0 else behind},
            device_id_type=MESH,
        )

    def add_and_send(slot, flow, piece, step, incoming):
        lo, size = ospans[piece]
        cols = pl.ds(lo, size)
        total = mine[slot, :, cols].astype(f32) + pin[slot, :, cols].astype(f32)
        if incoming:
            sum_copy(slot, flow, piece, step - 1).wait_recv()
            total = total + rsin[flow, step - 1, :, cols].astype(f32)
        mine[slot, :, cols] = total.astype(bf16)
        sum_copy(slot, flow, piece, step).start()

    give(0).wait_recv()
    for flow in range(2):
        add_and_send(1, flow, flow, 0, False)
    give(last).wait_recv()
    for flow in range(2):
        add_and_send(2 * last + flow, flow, 1 - flow, 1, False)
    for flow in range(2):
        add_and_send(2 * last + flow, flow, flow, 1, True)

    def fold(step, carry):
        s = half - step
        give(s).wait_recv()
        for piece in range(2):
            for flow in range(2):
                add_and_send(2 * s + flow, flow, piece, step, True)
        return carry

    lax.fori_loop(2, half, fold, 0)

    for piece in range(2):
        lo, size = ospans[piece]
        cols = pl.ds(lo, size)
        total = resid_ref[:, cols] + mine[0, :, cols].astype(f32) + pin[0, :, cols].astype(f32)
        for flow in range(2):
            sum_copy(0, flow, piece, half - 1).wait_recv()
            total = total + rsin[flow, half - 1, :, cols].astype(f32)
        out_ref[:, cols] = total.astype(bf16)

    def drain_ring(s, carry):
        for flow in range(2):
            for piece in range(2):
                ring_copy(x_ref, 1, flow, piece, s).wait_send()
        return carry

    lax.fori_loop(1, half, drain_ring, 0)
    for flow in range(2):
        ring_copy(x_ref, 1, flow, flow, half).wait_send()

    def drain_slots(slot, carry):
        for piece in range(2):
            partner_copy(x_ref, slot, piece).wait_send()
        return carry

    lax.fori_loop(0, ring, drain_slots, 0)

    def drain_groups(g, carry):
        give(g).wait_send()
        return carry

    lax.fori_loop(0, half, drain_groups, 0)

    def drain_sums(step, carry):
        for flow in range(2):
            for piece in range(2):
                sum_copy(0, flow, piece, step).wait_send()
        return carry

    for flow in range(2):
        sum_copy(0, flow, flow, 0).wait_send()
    lax.fori_loop(1, half, drain_sums, 0)


def expert_layer(x_wide, resid, w_gate, w_up, w_down):
    ring = lax.axis_size("tok")
    half = ring // 2
    block, width = resid.shape
    ffs = w_gate.shape[1]
    wide = x_wide.shape[1]
    vmem = pl.BlockSpec(memory_space=pltpu.VMEM)
    hbm = pl.BlockSpec(memory_space=pl.ANY)
    dma = pltpu.SemaphoreType.DMA
    return pl.pallas_call(
        functools.partial(expert_kernel, half),
        out_shape=jax.ShapeDtypeStruct((block, width), bf16),
        in_specs=[vmem, vmem, hbm, hbm, hbm],
        out_specs=vmem,
        scratch_shapes=[
            pltpu.VMEM((ring, 2, block, wide), bf16),
            pltpu.VMEM((width, 2 * ffs), bf16),
            pltpu.VMEM((ffs, width), bf16),
            pltpu.VMEM((4 * block, 2 * ffs), f32),
            pltpu.VMEM((4 * block, ffs), bf16),
            pltpu.VMEM((ring, block, width), bf16),
            pltpu.VMEM((ring, block, width), bf16),
            pltpu.VMEM((ring, block, width), bf16),
            pltpu.VMEM((2, half, block, width), bf16),
            dma((3,)),
            dma((half + 1, 2, 2)),
            dma((half + 1, 2, 2)),
            dma((ring, 2)),
            dma((ring, 2)),
            dma((half,)),
            dma((half,)),
            dma((half, 2, 2)),
            dma((half, 2, 2)),
        ],
        compiler_params=pltpu.CompilerParams(
            collective_id=1, has_side_effects=True, vmem_limit_bytes=67043328
        ),
        name="expert_layer",
    )(x_wide, resid, w_gate, w_up, w_down)


def shards(
    hidden,
    queries,
    cache,
    cache_lengths,
    wkv,
    wo,
    attn_gain,
    moe_gain,
    w_gate,
    w_up,
    w_down,
    expert_ids,
    gates,
):
    full_rows = collect(hidden, "mdl", 1)
    span_len = full_rows.shape[0]
    normalized_input = rms_scale(full_rows, attn_gain).astype(jnp.bfloat16)
    kv_heads = wkv.shape[1]
    head_dim = wkv.shape[3]
    weight_piece = lax.all_gather(wkv, "tok", axis=0, tiled=True)
    key_value_projection = jnp.dot(
        normalized_input,
        weight_piece.reshape(weight_piece.shape[0], -1),
        preferred_element_type=jnp.float32,
    ).reshape(span_len, kv_heads, 2, head_dim)
    length = cache_lengths[0]
    positions = length + jnp.arange(span_len, dtype=jnp.int32)
    fresh_key_value = jnp.stack(
        [rotate(key_value_projection[:, :, 0], positions), key_value_projection[:, :, 1]], axis=2
    ).astype(jnp.bfloat16)
    head_group = queries.shape[1] // kv_heads
    outputs = []
    for head_index in range(kv_heads):
        query_rows = queries[:, head_index * head_group : (head_index + 1) * head_group].reshape(
            span_len * head_group, head_dim
        )
        attended = head_attention(
            query_rows,
            cache[0, :, head_index, 0],
            cache[0, :, head_index, 1],
            length,
            fresh_key_value[:, head_index, 0],
            fresh_key_value[:, head_index, 1],
            head_group,
        )
        outputs.append(attended.reshape(span_len, head_group * head_dim))
    heads_out = jnp.concatenate(outputs, axis=1)
    weight_piece = lax.all_gather(wo, "tok", axis=2, tiled=True)
    attn_out = jnp.dot(
        heads_out,
        weight_piece.reshape(-1, weight_piece.shape[2]),
        preferred_element_type=jnp.float32,
    )
    core_rows = span_len // lax.axis_size("mdl")
    core_start = lax.axis_index("mdl") * core_rows
    attn_rows = sent_and_summed(attn_out, "mdl", 0)
    resid = (
        lax.dynamic_slice_in_dim(full_rows, core_start, core_rows, 0).astype(jnp.float32)
        + attn_rows
    )
    moe_in = rms_scale(resid, moe_gain).astype(jnp.bfloat16)
    matches = expert_ids[:, :, None] == jnp.arange(EXPERTS)[None, None, :]
    route = jnp.sum(jnp.where(matches, gates[:, :, None], 0.0), axis=1)
    high = route.astype(bf16)
    low = (route - high.astype(f32)).astype(bf16)
    pad = jnp.zeros((core_rows, LANES - 2 * EXPERTS), bf16)
    x_wide = jnp.concatenate([moe_in, high, low, pad], axis=1)
    mixed = expert_layer(x_wide, resid, w_gate[0], w_up[0], w_down[0])
    return (mixed, fresh_key_value)


def solution(mesh):
    in_specs = (
        P(("grp", "tok"), "mdl"),
        P(("grp", "tok"), "mdl", None),
        P(("grp", "tok"), None, "mdl", None, None),
        P(("grp", "tok")),
        P("tok", "mdl", None, None),
        P("mdl", None, "tok"),
        P(),
        P(),
        P(("tok", "mdl"), None, None),
        P(("tok", "mdl"), None, None),
        P(("tok", "mdl"), None, None),
        P(("grp", "tok", "mdl"), None),
        P(("grp", "tok", "mdl"), None),
    )
    out_specs = (P(("grp", "tok", "mdl"), None), P(("grp", "tok"), "mdl", None, None))
    return jax.shard_map(shards, mesh=mesh, in_specs=in_specs, out_specs=out_specs, check_vma=False)
```

```python
import functools
import math

import jax
import jax.numpy as jnp
from jax import lax
from jax.experimental import pallas as pl
from jax.experimental.pallas import tpu as pltpu
from jax.sharding import PartitionSpec as P

EXPERTS = 4
TOPK = 2

eps_norm = 1e-05
rope_base = 1000000.0
mask_fill = -1e30

MESH = pl.DeviceIdType.MESH
bf16 = jnp.bfloat16
f32 = jnp.float32


LANES = 128
KEYS = 512


def permutation(groups, size):
    each = size // groups
    row = lax.broadcasted_iota(jnp.int32, (size, size), 0)
    col = lax.broadcasted_iota(jnp.int32, (size, size), 1)
    return jnp.where(col == lax.rem(row, each) * groups + row // each, 1.0, 0.0).astype(bf16)


def prelude_kernel(
    half,
    side,
    hid_ref,
    q_ref,
    cache_hbm,
    len_ref,
    wkv_ref,
    wo_ref,
    again_ref,
    mgain_ref,
    ids_ref,
    gates_ref,
    x_ref,
    resid_ref,
    fresh_ref,
    hfull,
    normed,
    kvbuf,
    wobuf,
    raw,
    keys,
    vals,
    qs,
    kvacc,
    smax,
    ssum,
    sacc,
    heads,
    part,
    part_in,
    csem,
    h_send,
    h_recv,
    kv_send,
    kv_recv,
    kvn_send,
    kvn_recv,
    wo_send,
    wo_recv,
    won_send,
    won_recv,
    p_send,
    p_recv,
):
    ring = 2 * half
    z = lax.axis_index("tok")
    m = lax.axis_index("mdl")
    gid = lax.axis_index("grp")
    ahead = lax.rem(z + 1, ring)
    behind = lax.rem(z + ring - 1, ring)
    odd_a = lax.rem(gid // side, 2)
    odd_b = lax.rem(gid, 2)
    neighbours = ({"grp": gid + side * (1 - 2 * odd_a)}, {"grp": gid + 1 - 2 * odd_b})
    own = 2 * odd_a + odd_b
    quarters = (own, 3 - own)
    partner = {"mdl": 1 - m}
    span, wide_half = hid_ref.shape
    block = span // 2
    width = resid_ref.shape[1]
    chip_cols = width // ring
    kv_heads = keys.shape[0]
    positions = keys.shape[1]
    head_total, _, head_dim = qs.shape
    per_group = head_total // kv_heads
    rows = per_group * span
    scale = 1.0 / math.sqrt(head_dim)

    load = pltpu.make_async_copy(cache_hbm, raw, csem.at[0])
    load.start()

    barrier = pltpu.get_barrier_semaphore()
    for who in ({"tok": ahead}, {"tok": behind}, *neighbours, partner):
        pl.semaphore_signal(barrier, inc=1, device_id=who, device_id_type=MESH)

    four = 2 * kv_heads
    perm4 = permutation(four, 64 * four)
    for q in range(4):
        got = jnp.dot(perm4, wkv_ref[q], preferred_element_type=f32).astype(bf16)
        for j in range(four):
            kvbuf[0, q, :, pl.ds(j * head_dim, head_dim)] = got[j * 64 : (j + 1) * 64]
    pl.semaphore_wait(barrier, 5)

    hid_copy = pltpu.make_async_remote_copy(
        src_ref=hid_ref,
        dst_ref=hfull.at[m],
        send_sem=h_send.at[0],
        recv_sem=h_recv.at[0],
        device_id=partner,
        device_id_type=MESH,
    )
    hid_copy.start()

    kinds = {
        "kv": (kvbuf, kv_send, kv_recv, kvn_send, kvn_recv),
        "wo": (wobuf, wo_send, wo_recv, won_send, won_recv),
    }

    def slot_of(step, flow):
        return 1 if isinstance(step, int) and step == half else 2 * step + flow

    def ring_copy(kind, src, step, flow, piece):
        buf, send, recv, _, _ = kinds[kind]
        q = quarters[piece]
        return pltpu.make_async_remote_copy(
            src_ref=src.at[q],
            dst_ref=buf.at[slot_of(step, flow), q],
            send_sem=send.at[step, flow, piece],
            recv_sem=recv.at[step, flow, piece],
            device_id={"tok": behind if flow == 0 else ahead},
            device_id_type=MESH,
        )

    def side_copy(kind, slot, axis):
        buf, _, _, send, recv = kinds[kind]
        return pltpu.make_async_remote_copy(
            src_ref=buf.at[slot, own],
            dst_ref=buf.at[slot, own],
            send_sem=send.at[slot, axis],
            recv_sem=recv.at[slot, axis],
            device_id=neighbours[axis],
            device_id_type=MESH,
        )

    def arrive(kind, step):
        buf = kinds[kind][0]
        for piece in range(2):
            for flow in range(2):
                final = isinstance(step, int) and step == half
                if final and flow != piece:
                    continue
                slot = slot_of(step, flow)
                ring_copy(kind, buf.at[slot], step, flow, piece).wait_recv()
                if not final:
                    turn = isinstance(step, int) and step == half - 1
                    if not turn or flow == piece:
                        ring_copy(kind, buf.at[slot], step + 1, flow, piece).start()
                if piece == 0:
                    for axis in range(2):
                        side_copy(kind, slot, axis).start()

    def settle(kind, slot):
        for axis in range(2):
            side_copy(kind, slot, axis).wait_recv()

    for piece in range(2):
        for flow in range(2):
            ring_copy("kv", kvbuf.at[0], 1, flow, piece).start()
    for piece in range(2):
        for flow in range(2):
            ring_copy("wo", wo_ref, 1, flow, piece).start()

    lane = lax.broadcasted_iota(jnp.int32, (16, block), 0)
    route = jnp.zeros((16, block), f32)
    for k in range(TOPK):
        hit = (ids_ref[k : k + 1, :] == lane) | (ids_ref[k : k + 1, :] + EXPERTS == lane)
        route = route + jnp.where(hit, gates_ref[k : k + 1, :], 0.0)
    high = route.astype(bf16).astype(f32)
    terms = jnp.where(lane < EXPERTS, high, route - high)
    place = lax.broadcasted_iota(jnp.int32, (16, LANES), 0) == lax.broadcasted_iota(
        jnp.int32, (16, LANES), 1
    )
    tail = lax.dot_general(
        terms.astype(bf16),
        jnp.where(place, 1.0, 0.0).astype(bf16),
        (((0,), (0,)), ((), ())),
        preferred_element_type=f32,
    )
    x_ref[:, pl.ds(width, LANES)] = tail.astype(bf16)

    perm_q = permutation(head_total, 32 * head_total)
    for b in range(span // 32):
        got = jnp.dot(perm_q, q_ref[b], preferred_element_type=f32).astype(bf16)
        for h in range(head_total):
            qs[h, pl.ds(32 * b, 32), :] = got[32 * h : 32 * (h + 1)]

    hfull[m] = hid_ref[...]
    hid_copy.wait_recv()
    square = jnp.zeros((span, LANES), f32)
    for j in range(width // LANES):
        v = hfull[j // (ring // 2 * chip_cols // LANES), :, pl.ds(j * LANES % wide_half, LANES)]
        v = v.astype(f32)
        square = square + v * v
    inv = lax.rsqrt(jnp.sum(square, axis=1, keepdims=True) / width + eps_norm)
    for c in range(ring):
        v = hfull[c * chip_cols // wide_half, :, pl.ds(c * chip_cols % wide_half, chip_cols)]
        gain = again_ref[:, pl.ds(c * chip_cols, chip_cols)].astype(f32)
        normed[c] = (v.astype(f32) * inv * gain).astype(bf16)

    def chip_of(slot):
        if isinstance(slot, int) and slot < 2:
            return lax.rem(z + slot * half, ring)
        step, flow = slot // 2, lax.rem(slot, 2)
        return lax.rem(z + ring + step * (1 - 2 * flow), ring)

    def kv_use(slot):
        weights = kvbuf[slot].reshape(chip_cols, four * head_dim)
        kvacc[...] += jnp.dot(normed[chip_of(slot)], weights, preferred_element_type=f32)

    kvacc[...] = jnp.zeros_like(kvacc)
    kv_use(0)

    load.wait()

    def unpack(b, carry):
        got = jnp.dot(
            perm4,
            raw[pl.ds(pl.multiple_of(b * 64 * four, 64 * four), 64 * four), :],
            preferred_element_type=f32,
        ).astype(bf16)
        at = pl.ds(pl.multiple_of(b * 64, 64), 64)
        for g in range(kv_heads):
            keys[g, at, :] = got[(2 * g) * 64 : (2 * g + 1) * 64]
            vals[g, at, :] = got[(2 * g + 1) * 64 : (2 * g + 2) * 64]
        return carry

    lax.fori_loop(0, positions // 64, unpack, 0)

    length = len_ref[0]
    smax[...] = jnp.full_like(smax, mask_fill)
    ssum[...] = jnp.zeros_like(ssum)
    sacc[...] = jnp.zeros_like(sacc)

    def attend(g, key_rows, value_rows, allowed):
        query_rows = qs[pl.ds(per_group * g, per_group)].reshape(rows, head_dim)
        scores = lax.dot_general(
            query_rows, key_rows, (((1,), (1,)), ((), ())), preferred_element_type=f32
        )
        scores = jnp.where(allowed, scores * scale, mask_fill)
        old = smax[g][:, :1]
        top = jnp.maximum(old, jnp.max(scores, axis=1, keepdims=True))
        weights = jnp.where(allowed, jnp.exp(scores - top), 0.0)
        fade = jnp.exp(old - top)
        smax[g] = jnp.broadcast_to(top, (rows, LANES))
        ssum[g] = ssum[g] * fade + jnp.sum(weights, axis=1, keepdims=True)
        sacc[g] = sacc[g] * fade + jnp.dot(
            weights.astype(bf16), value_rows, preferred_element_type=f32
        )

    key_blocks = positions // KEYS

    def cached(i):
        g = i // key_blocks
        lo = lax.rem(i, key_blocks) * KEYS
        if not isinstance(lo, int):
            lo = pl.multiple_of(lo, KEYS)
        col = lo + lax.broadcasted_iota(jnp.int32, (rows, KEYS), 1)
        attend(g, keys[g, pl.ds(lo, KEYS), :], vals[g, pl.ds(lo, KEYS), :], col < length)

    def kv_step(step):
        arrive("kv", step)
        cached(step - 1)

    def kv_settled(step):
        for flow in range(2):
            settle("kv", slot_of(step, flow))
            kv_use(slot_of(step, flow))

    kv_step(1)

    def pair(k):
        kv_step(2 * k)
        kv_settled(2 * k - 1)
        arrive("wo", k)
        kv_step(2 * k + 1)
        kv_settled(2 * k)

    def pairs(k, carry):
        pair(k)
        return carry

    lax.fori_loop(1, half // 2 - 1, pairs, 0)
    pair(half // 2 - 1)
    arrive("kv", half)
    kv_settled(half - 1)
    cached(jnp.int32(half - 1))
    arrive("wo", half // 2)
    settle("kv", 1)
    kv_use(1)

    lanes = lax.broadcasted_iota(jnp.int32, (span, head_dim), 1)
    place_of = lax.broadcasted_iota(jnp.int32, (span, head_dim), 0) + length
    pair_of = lax.rem(lanes, head_dim // 2).astype(f32)
    angle = place_of.astype(f32) * jnp.exp(pair_of * (-2.0 * math.log(rope_base) / head_dim))
    cosine = jnp.cos(angle)
    sine = jnp.where(lanes < head_dim // 2, -jnp.sin(angle), jnp.sin(angle))
    token = lax.rem(lax.broadcasted_iota(jnp.int32, (rows, span), 0), span)
    causal = lax.broadcasted_iota(jnp.int32, (rows, span), 1) <= token
    for g in range(kv_heads):
        k_cols = pl.ds(2 * g * head_dim, head_dim)
        v_cols = pl.ds((2 * g + 1) * head_dim, head_dim)
        key = kvacc[:, k_cols]
        turned = pltpu.roll(key, head_dim // 2, 1)
        fresh_ref[:, k_cols] = (key * cosine + turned * sine).astype(bf16)
        fresh_ref[:, v_cols] = kvacc[:, v_cols].astype(bf16)
        attend(g, fresh_ref[:, k_cols], fresh_ref[:, v_cols], causal)
        done = (sacc[g] / ssum[g]).astype(bf16)
        for h in range(per_group):
            at = pl.ds((g * per_group + h) * head_dim, head_dim)
            heads[:, at] = done[h * span : (h + 1) * span]

    def wo_use(slot, buf):
        weights = buf.reshape(4 * wo_ref.shape[1], chip_cols)
        got = jnp.dot(heads[...], weights, preferred_element_type=f32)
        for core in range(2):
            part[core, slot] = got[core * block : (core + 1) * block]

    def part_copy(g):
        return pltpu.make_async_remote_copy(
            src_ref=part.at[1 - m, pl.ds(2 * g, 2)],
            dst_ref=part_in.at[pl.ds(2 * g, 2)],
            send_sem=p_send.at[g],
            recv_sem=p_recv.at[g],
            device_id=partner,
            device_id_type=MESH,
        )

    def wo_settled(step):
        for flow in range(2):
            slot = slot_of(step, flow)
            settle("wo", slot)
            wo_use(slot, wobuf[slot])
        part_copy(step).start()

    def assemble(slot):
        c = chip_of(slot)
        cols = pl.ds(pl.multiple_of(c * chip_cols, chip_cols), chip_cols)
        in_half = pl.ds(
            pl.multiple_of(lax.rem(c * chip_cols, wide_half), chip_cols), chip_cols
        )
        mine = hfull[c * chip_cols // wide_half, pl.ds(pl.multiple_of(m * block, block), block), in_half]
        resid_ref[:, cols] = mine.astype(f32) + part[m, slot] + part_in[slot]

    def gather_parts(step):
        part_copy(step).wait_recv()
        for flow in range(2):
            assemble(slot_of(step, flow))

    wo_use(0, wo_ref[...])

    def late(s, carry):
        arrive("wo", s)
        first = 2 * (s - half // 2) - 1
        wo_settled(first)
        wo_settled(first + 1)
        return carry

    lax.fori_loop(half // 2 + 1, half - 1, late, 0)
    arrive("wo", half - 1)
    wo_settled(half - 3)

    def early(step, carry):
        gather_parts(step)
        return carry

    lax.fori_loop(1, half - 3, early, 0)
    arrive("wo", half)
    wo_settled(half - 2)
    wo_settled(half - 1)
    lax.fori_loop(half - 3, half, early, 0)
    settle("wo", 1)
    wo_use(1, wobuf[1])
    part_copy(0).start()
    part_copy(0).wait_recv()
    assemble(0)
    assemble(1)

    square = jnp.zeros((block, LANES), f32)
    for j in range(width // LANES):
        v = resid_ref[:, pl.ds(j * LANES, LANES)]
        square = square + v * v
    inv = lax.rsqrt(jnp.sum(square, axis=1, keepdims=True) / width + eps_norm)
    for c in range(ring):
        cols = pl.ds(c * chip_cols, chip_cols)
        gain = mgain_ref[:, cols].astype(f32)
        x_ref[:, cols] = (resid_ref[:, cols] * inv * gain).astype(bf16)

    hid_copy.wait_send()

    def drain_ring(step, carry):
        for kind in ("kv", "wo"):
            for flow in range(2):
                for piece in range(2):
                    ring_copy(kind, kinds[kind][0].at[0], step, flow, piece).wait_send()
        return carry

    lax.fori_loop(1, half, drain_ring, 0)
    for kind in ("kv", "wo"):
        for flow in range(2):
            ring_copy(kind, kinds[kind][0].at[0], half, flow, flow).wait_send()

    def drain_sides(slot, carry):
        for kind in ("kv", "wo"):
            for axis in range(2):
                side_copy(kind, slot, axis).wait_send()
        return carry

    lax.fori_loop(1, ring, drain_sides, 0)

    def drain_parts(g, carry):
        part_copy(g).wait_send()
        return carry

    lax.fori_loop(0, half, drain_parts, 0)


def prelude(hidden, queries, cache, cache_lengths, wkv, wo, attn_gain, moe_gain, expert_ids, gates):
    ring = lax.axis_size("tok")
    half = ring // 2
    side = math.isqrt(lax.axis_size("grp"))
    span, wide_half = hidden.shape
    block, width = span // 2, 2 * wide_half
    heads, head_dim = queries.shape[1:]
    positions, kv_heads = cache.shape[1:3]
    four = 2 * kv_heads
    chip_cols = width // ring
    rows = heads // kv_heads * span
    vmem = pl.BlockSpec(memory_space=pltpu.VMEM)
    hbm = pl.BlockSpec(memory_space=pl.ANY)
    smem = pl.BlockSpec(memory_space=pltpu.SMEM)
    dma = pltpu.SemaphoreType.DMA
    depth = heads * head_dim // 4
    return pl.pallas_call(
        functools.partial(prelude_kernel, half, side),
        out_shape=(
            jax.ShapeDtypeStruct((block, width + LANES), bf16),
            jax.ShapeDtypeStruct((block, width), f32),
            jax.ShapeDtypeStruct((span, four * head_dim), bf16),
        ),
        in_specs=[vmem, vmem, hbm, smem, vmem, vmem, vmem, vmem, vmem, vmem],
        out_specs=(vmem, vmem, vmem),
        scratch_shapes=[
            pltpu.VMEM((2, span, wide_half), bf16),
            pltpu.VMEM((ring, span, chip_cols), bf16),
            pltpu.VMEM((ring, 4, chip_cols // 4, four * head_dim), bf16),
            pltpu.VMEM((ring, 4, depth, chip_cols), bf16),
            pltpu.VMEM((positions * four, head_dim), bf16),
            pltpu.VMEM((kv_heads, positions, head_dim), bf16),
            pltpu.VMEM((kv_heads, positions, head_dim), bf16),
            pltpu.VMEM((heads, span, head_dim), bf16),
            pltpu.VMEM((span, four * head_dim), f32),
            pltpu.VMEM((kv_heads, rows, LANES), f32),
            pltpu.VMEM((kv_heads, rows, LANES), f32),
            pltpu.VMEM((kv_heads, rows, head_dim), f32),
            pltpu.VMEM((span, heads * head_dim), bf16),
            pltpu.VMEM((2, ring, block, chip_cols), f32),
            pltpu.VMEM((ring, block, chip_cols), f32),
            dma((1,)),
            dma((1,)),
            dma((1,)),
            dma((half + 1, 2, 2)),
            dma((half + 1, 2, 2)),
            dma((ring, 2)),
            dma((ring, 2)),
            dma((half + 1, 2, 2)),
            dma((half + 1, 2, 2)),
            dma((ring, 2)),
            dma((ring, 2)),
            dma((half,)),
            dma((half,)),
        ],
        compiler_params=pltpu.CompilerParams(
            collective_id=0, has_side_effects=True, vmem_limit_bytes=56 * 1024 * 1024
        ),
        name="prelude",
    )(
        hidden,
        queries.reshape(span // 32, 32 * heads, head_dim),
        cache.reshape(positions * four, head_dim),
        cache_lengths,
        wkv.reshape(4, chip_cols // 4 * four, head_dim),
        wo.reshape(4, depth, chip_cols),
        attn_gain.reshape(1, width),
        moe_gain.reshape(1, width),
        expert_ids.T,
        gates.T,
    )


GT = 256
DT = 512


def expert_kernel(
    half,
    x_ref,
    resid_ref,
    wg_hbm,
    wu_hbm,
    wd_hbm,
    out_ref,
    xs,
    wgu,
    wd,
    gu,
    hid,
    mine,
    pout,
    pin,
    rsin,
    wsem,
    ag_send,
    ag_recv,
    x_send,
    x_recv,
    p_send,
    p_recv,
    rs_send,
    rs_recv,
):
    ring = 2 * half
    z = lax.axis_index("tok")
    m = lax.axis_index("mdl")
    ahead = lax.rem(z + 1, ring)
    behind = lax.rem(z + ring - 1, ring)
    partner = {"mdl": 1 - m}
    expert = z // (ring // EXPERTS)
    block, width = resid_ref.shape
    ffs = wg_hbm.shape[1]
    wide = x_ref.shape[1]
    cut = width // 2
    spans = ((0, cut), (cut, wide - cut))
    ospans = ((0, cut), (cut, width - cut))

    loads = (
        pltpu.make_async_copy(wg_hbm, wgu.at[:, pl.ds(0, ffs)], wsem.at[0]),
        pltpu.make_async_copy(wu_hbm, wgu.at[:, pl.ds(ffs, ffs)], wsem.at[1]),
        pltpu.make_async_copy(wd_hbm, wd, wsem.at[2]),
    )

    barrier = pltpu.get_barrier_semaphore()
    for who in ({"tok": ahead}, {"tok": behind}, partner):
        pl.semaphore_signal(barrier, inc=1, device_id=who, device_id_type=MESH)
    pl.semaphore_wait(barrier, 3)

    def ring_copy(src, dst_slot, flow, piece, step):
        lo, size = spans[piece]
        return pltpu.make_async_remote_copy(
            src_ref=src.at[:, pl.ds(lo, size)],
            dst_ref=xs.at[dst_slot, 0, :, pl.ds(lo, size)],
            send_sem=ag_send.at[step, flow, piece],
            recv_sem=ag_recv.at[step, flow, piece],
            device_id={"tok": behind if flow == 0 else ahead},
            device_id_type=MESH,
        )

    def partner_copy(src, slot, piece):
        lo, size = spans[piece]
        return pltpu.make_async_remote_copy(
            src_ref=src.at[:, pl.ds(lo, size)],
            dst_ref=xs.at[slot, 1, :, pl.ds(lo, size)],
            send_sem=x_send.at[slot, piece],
            recv_sem=x_recv.at[slot, piece],
            device_id=partner,
            device_id_type=MESH,
        )

    def first_slot(flow, piece):
        return 2 + flow if half > 1 else 1

    for piece in range(2):
        for flow in range(2):
            ring_copy(x_ref, 2 + flow, flow, piece, 1).start()
    for load in loads:
        load.start()
    for piece in range(2):
        partner_copy(x_ref, 0, piece).start()
    xs[0, 0] = x_ref[...]

    def gate_up(g, lo, hi):
        def tile(n, carry):
            cols = pl.ds(pl.multiple_of(n * GT, GT), GT)
            rows = xs[pl.ds(2 * g, 2), :, :, pl.ds(0, width)].reshape(4 * block, width)
            gu[:, cols] = jnp.dot(rows, wgu[:, cols], preferred_element_type=f32)
            return carry

        lax.fori_loop(lo, hi, tile, 0)

    def activate():
        gate = gu[:, pl.ds(0, ffs)]
        up = gu[:, pl.ds(ffs, ffs)]
        hid[...] = (gate / (1.0 + jnp.exp(-gate)) * up).astype(bf16)

    def weight_of(g):
        tail = xs[pl.ds(2 * g, 2), :, :, pl.ds(width, LANES)].reshape(4 * block, LANES)
        lane = lax.broadcasted_iota(jnp.int32, (4 * block, LANES), 1)
        pick = (lane == expert) | (lane == expert + EXPERTS)
        return jnp.sum(jnp.where(pick, tail.astype(f32), 0.0), axis=1, keepdims=True)

    def down(g, lo, hi):
        weight = weight_of(g)

        def tile(n, carry):
            cols = pl.ds(pl.multiple_of(n * DT, DT), DT)
            got = jnp.dot(hid[...], wd[:, cols], preferred_element_type=f32) * weight
            got = got.astype(bf16)
            for slot in range(2):
                mine[2 * g + slot, :, cols] = got[2 * slot * block : (2 * slot + 1) * block]
                pout[2 * g + slot, :, cols] = got[(2 * slot + 1) * block : (2 * slot + 2) * block]
            return carry

        lax.fori_loop(lo, hi, tile, 0)

    gtiles = 2 * ffs // GT
    dtiles = width // DT

    def give(g):
        return pltpu.make_async_remote_copy(
            src_ref=pout.at[pl.ds(2 * g, 2)],
            dst_ref=pin.at[pl.ds(2 * g, 2)],
            send_sem=p_send.at[g],
            recv_sem=p_recv.at[g],
            device_id=partner,
            device_id_type=MESH,
        )

    def await_partner(g):
        for slot in range(2):
            for piece in range(2):
                partner_copy(x_ref, 2 * g + slot, piece).wait_recv()

    def arrive(s, flow, piece, onward):
        ring_copy(x_ref, 2 * s + flow, flow, piece, s).wait_recv()
        if onward is not None:
            ring_copy(xs.at[2 * s + flow, 0], onward, flow, piece, s + 1).start()
        partner_copy(xs.at[2 * s + flow, 0], 2 * s + flow, piece).start()

    def first_part(g):
        await_partner(g)
        gate_up(g, 0, gtiles)

    def second_part(g):
        activate()
        down(g, 0, dtiles)
        give(g).start()

    for flow in range(2):
        arrive(1, flow, 0, 4 + flow)
    for load in loads:
        load.wait()
    for flow in range(2):
        arrive(1, flow, 1, 4 + flow)

    def body(s, carry):
        for flow in range(2):
            arrive(s, flow, 0, 2 * (s + 1) + flow)
        first_part(s - 1)
        for flow in range(2):
            arrive(s, flow, 1, 2 * (s + 1) + flow)
        second_part(s - 1)
        return carry

    lax.fori_loop(2, half - 1, body, 0)

    last = half - 1
    arrive(last, 0, 0, 1)
    arrive(last, 1, 0, None)
    first_part(last - 1)
    arrive(last, 0, 1, None)
    arrive(last, 1, 1, 1)
    second_part(last - 1)

    await_partner(last)
    gate_up(last, 0, gtiles)
    for flow in range(2):
        ring_copy(x_ref, 1, flow, flow, half).wait_recv()
        partner_copy(xs.at[1, 0], 1, flow).start()
    second_part(last)
    await_partner(0)
    gate_up(0, 0, gtiles)
    activate()
    down(0, 0, dtiles)
    give(0).start()

    def sum_copy(slot, flow, piece, step):
        lo, size = ospans[piece]
        return pltpu.make_async_remote_copy(
            src_ref=mine.at[slot, :, pl.ds(lo, size)],
            dst_ref=rsin.at[flow, step, :, pl.ds(lo, size)],
            send_sem=rs_send.at[step, flow, piece],
            recv_sem=rs_recv.at[step, flow, piece],
            device_id={"tok": ahead if flow == 0 else behind},
            device_id_type=MESH,
        )

    def add_and_send(slot, flow, piece, step, incoming):
        lo, size = ospans[piece]
        cols = pl.ds(lo, size)
        total = mine[slot, :, cols].astype(f32) + pin[slot, :, cols].astype(f32)
        if incoming:
            sum_copy(slot, flow, piece, step - 1).wait_recv()
            total = total + rsin[flow, step - 1, :, cols].astype(f32)
        mine[slot, :, cols] = total.astype(bf16)
        sum_copy(slot, flow, piece, step).start()

    give(0).wait_recv()
    for flow in range(2):
        add_and_send(1, flow, flow, 0, False)
    give(last).wait_recv()
    for flow in range(2):
        add_and_send(2 * last + flow, flow, 1 - flow, 1, False)
    for flow in range(2):
        add_and_send(2 * last + flow, flow, flow, 1, True)

    def fold(step, carry):
        s = half - step
        give(s).wait_recv()
        for piece in range(2):
            for flow in range(2):
                add_and_send(2 * s + flow, flow, piece, step, True)
        return carry

    lax.fori_loop(2, half, fold, 0)

    for piece in range(2):
        lo, size = ospans[piece]
        cols = pl.ds(lo, size)
        total = resid_ref[:, cols] + mine[0, :, cols].astype(f32) + pin[0, :, cols].astype(f32)
        for flow in range(2):
            sum_copy(0, flow, piece, half - 1).wait_recv()
            total = total + rsin[flow, half - 1, :, cols].astype(f32)
        out_ref[:, cols] = total.astype(bf16)

    def drain_ring(s, carry):
        for flow in range(2):
            for piece in range(2):
                ring_copy(x_ref, 1, flow, piece, s).wait_send()
        return carry

    lax.fori_loop(1, half, drain_ring, 0)
    for flow in range(2):
        ring_copy(x_ref, 1, flow, flow, half).wait_send()

    def drain_slots(slot, carry):
        for piece in range(2):
            partner_copy(x_ref, slot, piece).wait_send()
        return carry

    lax.fori_loop(0, ring, drain_slots, 0)

    def drain_groups(g, carry):
        give(g).wait_send()
        return carry

    lax.fori_loop(0, half, drain_groups, 0)

    def drain_sums(step, carry):
        for flow in range(2):
            for piece in range(2):
                sum_copy(0, flow, piece, step).wait_send()
        return carry

    for flow in range(2):
        sum_copy(0, flow, flow, 0).wait_send()
    lax.fori_loop(1, half, drain_sums, 0)


def expert_layer(x_wide, resid, w_gate, w_up, w_down):
    ring = lax.axis_size("tok")
    half = ring // 2
    block, width = resid.shape
    ffs = w_gate.shape[1]
    wide = x_wide.shape[1]
    vmem = pl.BlockSpec(memory_space=pltpu.VMEM)
    hbm = pl.BlockSpec(memory_space=pl.ANY)
    dma = pltpu.SemaphoreType.DMA
    return pl.pallas_call(
        functools.partial(expert_kernel, half),
        out_shape=jax.ShapeDtypeStruct((block, width), bf16),
        in_specs=[vmem, vmem, hbm, hbm, hbm],
        out_specs=vmem,
        scratch_shapes=[
            pltpu.VMEM((ring, 2, block, wide), bf16),
            pltpu.VMEM((width, 2 * ffs), bf16),
            pltpu.VMEM((ffs, width), bf16),
            pltpu.VMEM((4 * block, 2 * ffs), f32),
            pltpu.VMEM((4 * block, ffs), bf16),
            pltpu.VMEM((ring, block, width), bf16),
            pltpu.VMEM((ring, block, width), bf16),
            pltpu.VMEM((ring, block, width), bf16),
            pltpu.VMEM((2, half, block, width), bf16),
            dma((3,)),
            dma((half + 1, 2, 2)),
            dma((half + 1, 2, 2)),
            dma((ring, 2)),
            dma((ring, 2)),
            dma((half,)),
            dma((half,)),
            dma((half, 2, 2)),
            dma((half, 2, 2)),
        ],
        compiler_params=pltpu.CompilerParams(
            collective_id=1, has_side_effects=True, vmem_limit_bytes=67043328
        ),
        name="expert_layer",
    )(x_wide, resid, w_gate, w_up, w_down)


def shards(
    hidden,
    queries,
    cache,
    cache_lengths,
    wkv,
    wo,
    attn_gain,
    moe_gain,
    w_gate,
    w_up,
    w_down,
    expert_ids,
    gates,
):
    x_wide, resid, fresh = prelude(
        hidden, queries, cache, cache_lengths, wkv, wo, attn_gain, moe_gain, expert_ids, gates
    )
    mixed = expert_layer(x_wide, resid, w_gate[0], w_up[0], w_down[0])
    fresh_key_value = fresh.reshape(fresh.shape[0], *wkv.shape[1:])
    return (mixed, fresh_key_value)


def solution(mesh):
    in_specs = (
        P(("grp", "tok"), "mdl"),
        P(("grp", "tok"), "mdl", None),
        P(("grp", "tok"), None, "mdl", None, None),
        P(("grp", "tok")),
        P("tok", "mdl", None, None),
        P("mdl", None, "tok"),
        P(),
        P(),
        P(("tok", "mdl"), None, None),
        P(("tok", "mdl"), None, None),
        P(("tok", "mdl"), None, None),
        P(("grp", "tok", "mdl"), None),
        P(("grp", "tok", "mdl"), None),
    )
    out_specs = (P(("grp", "tok", "mdl"), None), P(("grp", "tok"), "mdl", None, None))
    return jax.shard_map(shards, mesh=mesh, in_specs=in_specs, out_specs=out_specs, check_vma=False)
```

```python
import functools
import math

import jax
import jax.numpy as jnp
from jax import lax
from jax.experimental import pallas as pl
from jax.experimental.pallas import tpu as pltpu
from jax.sharding import PartitionSpec as P

EXPERTS = 4
TOPK = 2

eps_norm = 1e-05
rope_base = 1000000.0
mask_fill = -1e30

MESH = pl.DeviceIdType.MESH
bf16 = jnp.bfloat16
f32 = jnp.float32


LANES = 128
KEYS = 512


def permutation(groups, size):
    each = size // groups
    row = lax.broadcasted_iota(jnp.int32, (size, size), 0)
    col = lax.broadcasted_iota(jnp.int32, (size, size), 1)
    return jnp.where(col == lax.rem(row, each) * groups + row // each, 1.0, 0.0).astype(bf16)


def prelude_kernel(
    half,
    side,
    hid_ref,
    q_ref,
    cache_hbm,
    len_ref,
    wkv_ref,
    wo_ref,
    again_ref,
    mgain_ref,
    ids_ref,
    gates_ref,
    x_ref,
    resid_ref,
    fresh_ref,
    hfull,
    normed,
    kvbuf,
    wobuf,
    raw,
    keys,
    vals,
    qs,
    kvacc,
    smax,
    ssum,
    sacc,
    heads,
    part,
    part_in,
    csem,
    h_send,
    h_recv,
    kv_send,
    kv_recv,
    kvn_send,
    kvn_recv,
    wo_send,
    wo_recv,
    won_send,
    won_recv,
    p_send,
    p_recv,
):
    ring = 2 * half
    z = lax.axis_index("tok")
    m = lax.axis_index("mdl")
    gid = lax.axis_index("grp")
    ahead = lax.rem(z + 1, ring)
    behind = lax.rem(z + ring - 1, ring)
    odd_a = lax.rem(gid // side, 2)
    odd_b = lax.rem(gid, 2)
    neighbours = ({"grp": gid + side * (1 - 2 * odd_a)}, {"grp": gid + 1 - 2 * odd_b})
    own = 2 * odd_a + odd_b
    quarters = (own, 3 - own)
    partner = {"mdl": 1 - m}
    span, wide_half = hid_ref.shape
    block = span // 2
    width = resid_ref.shape[1]
    chip_cols = width // ring
    kv_heads = keys.shape[0]
    positions = keys.shape[1]
    head_total, _, head_dim = qs.shape
    per_group = head_total // kv_heads
    rows = per_group * span
    scale = 1.0 / math.sqrt(head_dim)

    load = pltpu.make_async_copy(cache_hbm, raw, csem.at[0])
    load.start()

    barrier = pltpu.get_barrier_semaphore()
    for who in ({"tok": ahead}, {"tok": behind}, *neighbours, partner):
        pl.semaphore_signal(barrier, inc=1, device_id=who, device_id_type=MESH)

    four = 2 * kv_heads
    perm4 = permutation(four, 64 * four)
    for q in range(4):
        got = jnp.dot(perm4, wkv_ref[q], preferred_element_type=f32).astype(bf16)
        for j in range(four):
            kvbuf[0, q, :, pl.ds(j * head_dim, head_dim)] = got[j * 64 : (j + 1) * 64]
    pl.semaphore_wait(barrier, 5)

    hid_copy = pltpu.make_async_remote_copy(
        src_ref=hid_ref,
        dst_ref=hfull.at[m],
        send_sem=h_send.at[0],
        recv_sem=h_recv.at[0],
        device_id=partner,
        device_id_type=MESH,
    )
    hid_copy.start()

    kinds = {
        "kv": (kvbuf, kv_send, kv_recv, kvn_send, kvn_recv),
        "wo": (wobuf, wo_send, wo_recv, won_send, won_recv),
    }

    def slot_of(step, flow):
        return 1 if isinstance(step, int) and step == half else 2 * step + flow

    def ring_copy(kind, src, step, flow, piece):
        buf, send, recv, _, _ = kinds[kind]
        q = quarters[piece]
        return pltpu.make_async_remote_copy(
            src_ref=src.at[q],
            dst_ref=buf.at[slot_of(step, flow), q],
            send_sem=send.at[step, flow, piece],
            recv_sem=recv.at[step, flow, piece],
            device_id={"tok": behind if flow == 0 else ahead},
            device_id_type=MESH,
        )

    def side_copy(kind, slot, axis):
        buf, _, _, send, recv = kinds[kind]
        return pltpu.make_async_remote_copy(
            src_ref=buf.at[slot, own],
            dst_ref=buf.at[slot, own],
            send_sem=send.at[slot, axis],
            recv_sem=recv.at[slot, axis],
            device_id=neighbours[axis],
            device_id_type=MESH,
        )

    def arrive(kind, step, pieces=(0, 1)):
        buf = kinds[kind][0]
        for piece in pieces:
            for flow in range(2):
                final = isinstance(step, int) and step == half
                if final and flow != piece:
                    continue
                slot = slot_of(step, flow)
                ring_copy(kind, buf.at[slot], step, flow, piece).wait_recv()
                if not final:
                    turn = isinstance(step, int) and step == half - 1
                    if not turn or flow == piece:
                        ring_copy(kind, buf.at[slot], step + 1, flow, piece).start()
                if piece == 0:
                    for axis in range(2):
                        side_copy(kind, slot, axis).start()

    def settle(kind, slot):
        for axis in range(2):
            side_copy(kind, slot, axis).wait_recv()

    for piece in range(2):
        for flow in range(2):
            ring_copy("kv", kvbuf.at[0], 1, flow, piece).start()
    for piece in range(2):
        for flow in range(2):
            ring_copy("wo", wo_ref, 1, flow, piece).start()

    lane = lax.broadcasted_iota(jnp.int32, (16, block), 0)
    route = jnp.zeros((16, block), f32)
    for k in range(TOPK):
        hit = (ids_ref[k : k + 1, :] == lane) | (ids_ref[k : k + 1, :] + EXPERTS == lane)
        route = route + jnp.where(hit, gates_ref[k : k + 1, :], 0.0)
    high = route.astype(bf16).astype(f32)
    terms = jnp.where(lane < EXPERTS, high, route - high)
    place = lax.broadcasted_iota(jnp.int32, (16, LANES), 0) == lax.broadcasted_iota(
        jnp.int32, (16, LANES), 1
    )
    tail = lax.dot_general(
        terms.astype(bf16),
        jnp.where(place, 1.0, 0.0).astype(bf16),
        (((0,), (0,)), ((), ())),
        preferred_element_type=f32,
    )
    x_ref[:, pl.ds(width, LANES)] = tail.astype(bf16)

    perm_q = permutation(head_total, 32 * head_total)
    for b in range(span // 32):
        got = jnp.dot(perm_q, q_ref[b], preferred_element_type=f32).astype(bf16)
        for h in range(head_total):
            qs[h, pl.ds(32 * b, 32), :] = got[32 * h : 32 * (h + 1)]

    def gain_of(ref, c):
        each = chip_cols // LANES
        gains = [ref[c * each + j : c * each + j + 1, :].astype(f32) for j in range(each)]
        return jnp.concatenate(gains, axis=1)

    hfull[m] = hid_ref[...]
    hid_copy.wait_recv()
    square = jnp.zeros((span, LANES), f32)
    for j in range(width // LANES):
        v = hfull[j // (ring // 2 * chip_cols // LANES), :, pl.ds(j * LANES % wide_half, LANES)]
        v = v.astype(f32)
        square = square + v * v
    inv = lax.rsqrt(jnp.sum(square, axis=1, keepdims=True) / width + eps_norm)
    for c in range(ring):
        v = hfull[c * chip_cols // wide_half, :, pl.ds(c * chip_cols % wide_half, chip_cols)]
        gain = gain_of(again_ref, c)
        normed[c] = (v.astype(f32) * inv * gain).astype(bf16)

    def chip_of(slot):
        if isinstance(slot, int) and slot < 2:
            return lax.rem(z + slot * half, ring)
        step, flow = slot // 2, lax.rem(slot, 2)
        return lax.rem(z + ring + step * (1 - 2 * flow), ring)

    def kv_use(slot):
        weights = kvbuf[slot].reshape(chip_cols, four * head_dim)
        kvacc[...] += jnp.dot(normed[chip_of(slot)], weights, preferred_element_type=f32)

    kvacc[...] = jnp.zeros_like(kvacc)
    kv_use(0)

    load.wait()

    def unpack(b, carry):
        got = jnp.dot(
            perm4,
            raw[pl.ds(pl.multiple_of(b * 64 * four, 64 * four), 64 * four), :],
            preferred_element_type=f32,
        ).astype(bf16)
        at = pl.ds(pl.multiple_of(b * 64, 64), 64)
        for g in range(kv_heads):
            keys[g, at, :] = got[(2 * g) * 64 : (2 * g + 1) * 64]
            vals[g, at, :] = got[(2 * g + 1) * 64 : (2 * g + 2) * 64]
        return carry

    lax.fori_loop(0, positions // 64, unpack, 0)

    length = len_ref[0]
    smax[...] = jnp.full_like(smax, mask_fill)
    ssum[...] = jnp.zeros_like(ssum)
    sacc[...] = jnp.zeros_like(sacc)

    def attend(g, key_rows, value_rows, allowed):
        query_rows = qs[pl.ds(per_group * g, per_group)].reshape(rows, head_dim)
        scores = lax.dot_general(
            query_rows, key_rows, (((1,), (1,)), ((), ())), preferred_element_type=f32
        )
        scores = jnp.where(allowed, scores * scale, mask_fill)
        old = smax[g][:, :1]
        top = jnp.maximum(old, jnp.max(scores, axis=1, keepdims=True))
        weights = jnp.where(allowed, jnp.exp(scores - top), 0.0)
        fade = jnp.exp(old - top)
        smax[g] = jnp.broadcast_to(top, (rows, LANES))
        ssum[g] = ssum[g] * fade + jnp.sum(weights, axis=1, keepdims=True)
        sacc[g] = sacc[g] * fade + jnp.dot(
            weights.astype(bf16), value_rows, preferred_element_type=f32
        )

    key_blocks = positions // KEYS

    def cached(i):
        g = i // key_blocks
        lo = lax.rem(i, key_blocks) * KEYS
        if not isinstance(lo, int):
            lo = pl.multiple_of(lo, KEYS)
        col = lo + lax.broadcasted_iota(jnp.int32, (rows, KEYS), 1)
        attend(g, keys[g, pl.ds(lo, KEYS), :], vals[g, pl.ds(lo, KEYS), :], col < length)

    def kv_step(step):
        arrive("kv", step)
        cached(step - 1)

    def kv_settled(step):
        for flow in range(2):
            settle("kv", slot_of(step, flow))
            kv_use(slot_of(step, flow))

    kv_step(1)
    arrive("wo", 1, (0,))

    def pair(k):
        kv_step(2 * k)
        arrive("wo", k, (1,))
        kv_settled(2 * k - 1)
        kv_step(2 * k + 1)
        arrive("wo", k + 1, (0,))
        kv_settled(2 * k)

    def pairs(k, carry):
        pair(k)
        return carry

    lax.fori_loop(1, half // 2 - 1, pairs, 0)
    pair(half // 2 - 1)
    arrive("kv", half)
    arrive("wo", half // 2, (1,))
    kv_settled(half - 1)
    cached(jnp.int32(half - 1))
    settle("kv", 1)
    kv_use(1)

    lanes = lax.broadcasted_iota(jnp.int32, (span, head_dim), 1)
    place_of = lax.broadcasted_iota(jnp.int32, (span, head_dim), 0) + length
    pair_of = lax.rem(lanes, head_dim // 2).astype(f32)
    angle = place_of.astype(f32) * jnp.exp(pair_of * (-2.0 * math.log(rope_base) / head_dim))
    cosine = jnp.cos(angle)
    sine = jnp.where(lanes < head_dim // 2, -jnp.sin(angle), jnp.sin(angle))
    token = lax.rem(lax.broadcasted_iota(jnp.int32, (rows, span), 0), span)
    causal = lax.broadcasted_iota(jnp.int32, (rows, span), 1) <= token
    for g in range(kv_heads):
        k_cols = pl.ds(2 * g * head_dim, head_dim)
        v_cols = pl.ds((2 * g + 1) * head_dim, head_dim)
        key = kvacc[:, k_cols]
        turned = pltpu.roll(key, head_dim // 2, 1)
        fresh_ref[:, k_cols] = (key * cosine + turned * sine).astype(bf16)
        fresh_ref[:, v_cols] = kvacc[:, v_cols].astype(bf16)
        attend(g, fresh_ref[:, k_cols], fresh_ref[:, v_cols], causal)
        done = (sacc[g] / ssum[g]).astype(bf16)
        for h in range(per_group):
            at = pl.ds((g * per_group + h) * head_dim, head_dim)
            heads[:, at] = done[h * span : (h + 1) * span]

    def wo_use(slot, buf):
        weights = buf.reshape(4 * wo_ref.shape[1], chip_cols)
        got = jnp.dot(heads[...], weights, preferred_element_type=f32)
        for core in range(2):
            part[core, slot] = got[core * block : (core + 1) * block]

    def part_copy(g):
        return pltpu.make_async_remote_copy(
            src_ref=part.at[1 - m, pl.ds(2 * g, 2)],
            dst_ref=part_in.at[pl.ds(2 * g, 2)],
            send_sem=p_send.at[g],
            recv_sem=p_recv.at[g],
            device_id=partner,
            device_id_type=MESH,
        )

    def wo_settled(step):
        for flow in range(2):
            slot = slot_of(step, flow)
            settle("wo", slot)
            wo_use(slot, wobuf[slot])
        part_copy(step).start()

    def assemble(slot):
        c = chip_of(slot)
        cols = pl.ds(pl.multiple_of(c * chip_cols, chip_cols), chip_cols)
        in_half = pl.ds(
            pl.multiple_of(lax.rem(c * chip_cols, wide_half), chip_cols), chip_cols
        )
        mine = hfull[c * chip_cols // wide_half, pl.ds(pl.multiple_of(m * block, block), block), in_half]
        resid_ref[:, cols] = mine.astype(f32) + part[m, slot] + part_in[slot]

    def gather_parts(step):
        part_copy(step).wait_recv()
        for flow in range(2):
            assemble(slot_of(step, flow))

    wo_use(0, wo_ref[...])

    def late(s, carry):
        arrive("wo", s)
        first = 2 * (s - half // 2) - 1
        wo_settled(first)
        wo_settled(first + 1)
        return carry

    lax.fori_loop(half // 2 + 1, half - 1, late, 0)
    arrive("wo", half - 1)
    wo_settled(half - 3)

    def early(step, carry):
        gather_parts(step)
        return carry

    lax.fori_loop(1, half - 3, early, 0)
    arrive("wo", half)
    wo_settled(half - 2)
    wo_settled(half - 1)
    lax.fori_loop(half - 3, half, early, 0)
    settle("wo", 1)
    wo_use(1, wobuf[1])
    part_copy(0).start()
    part_copy(0).wait_recv()
    assemble(0)
    assemble(1)

    square = jnp.zeros((block, LANES), f32)
    for j in range(width // LANES):
        v = resid_ref[:, pl.ds(j * LANES, LANES)]
        square = square + v * v
    inv = lax.rsqrt(jnp.sum(square, axis=1, keepdims=True) / width + eps_norm)
    for c in range(ring):
        cols = pl.ds(c * chip_cols, chip_cols)
        gain = gain_of(mgain_ref, c)
        x_ref[:, cols] = (resid_ref[:, cols] * inv * gain).astype(bf16)

    hid_copy.wait_send()

    def drain_ring(step, carry):
        for kind in ("kv", "wo"):
            for flow in range(2):
                for piece in range(2):
                    ring_copy(kind, kinds[kind][0].at[0], step, flow, piece).wait_send()
        return carry

    lax.fori_loop(1, half, drain_ring, 0)
    for kind in ("kv", "wo"):
        for flow in range(2):
            ring_copy(kind, kinds[kind][0].at[0], half, flow, flow).wait_send()

    def drain_sides(slot, carry):
        for kind in ("kv", "wo"):
            for axis in range(2):
                side_copy(kind, slot, axis).wait_send()
        return carry

    lax.fori_loop(1, ring, drain_sides, 0)

    def drain_parts(g, carry):
        part_copy(g).wait_send()
        return carry

    lax.fori_loop(0, half, drain_parts, 0)


def prelude(hidden, queries, cache, cache_lengths, wkv, wo, attn_gain, moe_gain, expert_ids, gates):
    ring = lax.axis_size("tok")
    half = ring // 2
    side = math.isqrt(lax.axis_size("grp"))
    span, wide_half = hidden.shape
    block, width = span // 2, 2 * wide_half
    heads, head_dim = queries.shape[1:]
    positions, kv_heads = cache.shape[1:3]
    four = 2 * kv_heads
    chip_cols = width // ring
    rows = heads // kv_heads * span
    vmem = pl.BlockSpec(memory_space=pltpu.VMEM)
    hbm = pl.BlockSpec(memory_space=pltpu.HBM)
    smem = pl.BlockSpec(memory_space=pltpu.SMEM)
    dma = pltpu.SemaphoreType.DMA
    depth = heads * head_dim // 4
    return pl.pallas_call(
        functools.partial(prelude_kernel, half, side),
        out_shape=(
            jax.ShapeDtypeStruct((block, width + LANES), bf16),
            jax.ShapeDtypeStruct((block, width), f32),
            jax.ShapeDtypeStruct((span, four * head_dim), bf16),
        ),
        in_specs=[vmem, vmem, hbm, smem, vmem, vmem, vmem, vmem, vmem, vmem],
        out_specs=(vmem, vmem, vmem),
        scratch_shapes=[
            pltpu.VMEM((2, span, wide_half), bf16),
            pltpu.VMEM((ring, span, chip_cols), bf16),
            pltpu.VMEM((ring, 4, chip_cols // 4, four * head_dim), bf16),
            pltpu.VMEM((ring, 4, depth, chip_cols), bf16),
            pltpu.VMEM((positions * four, head_dim), bf16),
            pltpu.VMEM((kv_heads, positions, head_dim), bf16),
            pltpu.VMEM((kv_heads, positions, head_dim), bf16),
            pltpu.VMEM((heads, span, head_dim), bf16),
            pltpu.VMEM((span, four * head_dim), f32),
            pltpu.VMEM((kv_heads, rows, LANES), f32),
            pltpu.VMEM((kv_heads, rows, LANES), f32),
            pltpu.VMEM((kv_heads, rows, head_dim), f32),
            pltpu.VMEM((span, heads * head_dim), bf16),
            pltpu.VMEM((2, ring, block, chip_cols), f32),
            pltpu.VMEM((ring, block, chip_cols), f32),
            dma((1,)),
            dma((1,)),
            dma((1,)),
            dma((half + 1, 2, 2)),
            dma((half + 1, 2, 2)),
            dma((ring, 2)),
            dma((ring, 2)),
            dma((half + 1, 2, 2)),
            dma((half + 1, 2, 2)),
            dma((ring, 2)),
            dma((ring, 2)),
            dma((half,)),
            dma((half,)),
        ],
        compiler_params=pltpu.CompilerParams(
            collective_id=0, has_side_effects=True, vmem_limit_bytes=67043328
        ),
        name="prelude",
    )(
        hidden,
        queries.reshape(span // 32, 32 * heads, head_dim),
        cache.reshape(positions * four, head_dim),
        cache_lengths,
        wkv.reshape(4, chip_cols // 4 * four, head_dim),
        wo.reshape(4, depth, chip_cols),
        attn_gain.reshape(width // LANES, LANES),
        moe_gain.reshape(width // LANES, LANES),
        expert_ids.T,
        gates.T,
    )


GT = 256
DT = 512
PIECES = 2


def expert_kernel(
    half,
    x_ref,
    resid_ref,
    wg_hbm,
    wu_hbm,
    wd_hbm,
    out_ref,
    xs,
    wgu,
    wd,
    gu,
    hid,
    mine,
    pout,
    pin,
    rsin,
    wsem,
    ag_send,
    ag_recv,
    x_send,
    x_recv,
    p_send,
    p_recv,
    rs_send,
    rs_recv,
):
    ring = 2 * half
    z = lax.axis_index("tok")
    m = lax.axis_index("mdl")
    ahead = lax.rem(z + 1, ring)
    behind = lax.rem(z + ring - 1, ring)
    partner = {"mdl": 1 - m}
    expert = z // (ring // EXPERTS)
    block, width = resid_ref.shape
    ffs = wg_hbm.shape[1]
    cut = width // PIECES
    spans = [(i * cut, cut) for i in range(PIECES)]
    wide_spans = spans[:-1] + [(width - cut, cut + LANES)]
    side_of = [i * 2 // PIECES for i in range(PIECES)]

    loads = (
        pltpu.make_async_copy(wg_hbm, wgu.at[:, pl.ds(0, ffs)], wsem.at[0]),
        pltpu.make_async_copy(wu_hbm, wgu.at[:, pl.ds(ffs, ffs)], wsem.at[1]),
        pltpu.make_async_copy(wd_hbm, wd, wsem.at[2]),
    )

    barrier = pltpu.get_barrier_semaphore()
    for who in ({"tok": ahead}, {"tok": behind}, partner):
        pl.semaphore_signal(barrier, inc=1, device_id=who, device_id_type=MESH)
    pl.semaphore_wait(barrier, 3)

    def ring_copy(src, dst_slot, flow, piece, step):
        cols = pl.ds(*wide_spans[piece])
        return pltpu.make_async_remote_copy(
            src_ref=src.at[:, cols],
            dst_ref=xs.at[dst_slot, 0, :, cols],
            send_sem=ag_send.at[step, flow, piece],
            recv_sem=ag_recv.at[step, flow, piece],
            device_id={"tok": behind if flow == 0 else ahead},
            device_id_type=MESH,
        )

    def partner_copy(src, slot, piece):
        cols = pl.ds(*wide_spans[piece])
        return pltpu.make_async_remote_copy(
            src_ref=src.at[:, cols],
            dst_ref=xs.at[slot, 1, :, cols],
            send_sem=x_send.at[slot, piece],
            recv_sem=x_recv.at[slot, piece],
            device_id=partner,
            device_id_type=MESH,
        )

    for piece in range(PIECES):
        for flow in range(2):
            ring_copy(x_ref, 2 + flow, flow, piece, 1).start()
    for load in loads:
        load.start()
    for piece in range(PIECES):
        partner_copy(x_ref, 0, piece).start()
    xs[0, 0] = x_ref[...]

    def gate_up(g, lo, hi):
        def tile(n, carry):
            cols = pl.ds(pl.multiple_of(n * GT, GT), GT)
            rows = xs[pl.ds(2 * g, 2), :, :, pl.ds(0, width)].reshape(4 * block, width)
            gu[:, cols] = jnp.dot(rows, wgu[:, cols], preferred_element_type=f32)
            return carry

        lax.fori_loop(lo, hi, tile, 0)

    def activate():
        gate = gu[:, pl.ds(0, ffs)]
        up = gu[:, pl.ds(ffs, ffs)]
        hid[...] = (gate / (1.0 + jnp.exp(-gate)) * up).astype(bf16)

    def weight_of(g):
        tail = xs[pl.ds(2 * g, 2), :, :, pl.ds(width, LANES)].reshape(4 * block, LANES)
        lane = lax.broadcasted_iota(jnp.int32, (4 * block, LANES), 1)
        pick = (lane == expert) | (lane == expert + EXPERTS)
        return jnp.sum(jnp.where(pick, tail.astype(f32), 0.0), axis=1, keepdims=True)

    def down(g, lo, hi):
        weight = weight_of(g)

        def tile(n, carry):
            cols = pl.ds(pl.multiple_of(n * DT, DT), DT)
            got = jnp.dot(hid[...], wd[:, cols], preferred_element_type=f32) * weight
            got = got.astype(bf16)
            for slot in range(2):
                mine[2 * g + slot, :, cols] = got[2 * slot * block : (2 * slot + 1) * block]
                pout[2 * g + slot, :, cols] = got[(2 * slot + 1) * block : (2 * slot + 2) * block]
            return carry

        lax.fori_loop(lo, hi, tile, 0)

    gtiles = 2 * ffs // GT
    dtiles = width // DT

    def give(g, side):
        cols = pl.ds(side * (width // 2), width // 2)
        return pltpu.make_async_remote_copy(
            src_ref=pout.at[pl.ds(2 * g, 2), :, cols],
            dst_ref=pin.at[pl.ds(2 * g, 2), :, cols],
            send_sem=p_send.at[g, side],
            recv_sem=p_recv.at[g, side],
            device_id=partner,
            device_id_type=MESH,
        )

    def await_partner(g):
        for slot in range(2):
            for piece in range(PIECES):
                partner_copy(x_ref, 2 * g + slot, piece).wait_recv()

    def arrive(s, flow, piece, onward):
        ring_copy(x_ref, 2 * s + flow, flow, piece, s).wait_recv()
        if onward is not None:
            ring_copy(xs.at[2 * s + flow, 0], onward, flow, piece, s + 1).start()
        partner_copy(xs.at[2 * s + flow, 0], 2 * s + flow, piece).start()

    def parts(g):
        def first():
            await_partner(g)
            gate_up(g, 0, gtiles // 2)

        def second():
            gate_up(g, gtiles // 2, gtiles)

        def third():
            activate()
            down(g, 0, dtiles // 2)
            give(g, 0).start()

        def fourth():
            down(g, dtiles // 2, dtiles)
            give(g, 1).start()

        return first, second, third, fourth

    def spread(todo, piece):
        for i, part in enumerate(todo):
            if i * PIECES // 4 == piece:
                part()

    for piece in range(PIECES):
        for flow in range(2):
            arrive(1, flow, piece, 4 + flow)
        if piece == 0:
            for load in loads:
                load.wait()

    def body(s, carry):
        todo = parts(s - 1)
        for piece in range(PIECES):
            for flow in range(2):
                arrive(s, flow, piece, 2 * (s + 1) + flow)
            spread(todo, piece)
        return carry

    lax.fori_loop(2, half - 1, body, 0)

    last = half - 1
    todo = parts(last - 1)
    for piece in range(PIECES):
        for flow in range(2):
            arrive(last, flow, piece, 1 if flow == side_of[piece] else None)
        spread(todo, piece)

    todo = parts(last)
    order = [i // 2 + (i % 2) * (PIECES // 2) for i in range(PIECES)]
    for i, piece in enumerate(order):
        ring_copy(x_ref, 1, side_of[piece], piece, half).wait_recv()
        partner_copy(xs.at[1, 0], 1, piece).start()
        spread(todo, i)
    for part in parts(0):
        part()

    def sum_copy(slot, flow, piece, step):
        cols = pl.ds(*spans[piece])
        return pltpu.make_async_remote_copy(
            src_ref=mine.at[slot, :, cols],
            dst_ref=rsin.at[flow, step, :, cols],
            send_sem=rs_send.at[step, flow, piece],
            recv_sem=rs_recv.at[step, flow, piece],
            device_id={"tok": ahead if flow == 0 else behind},
            device_id_type=MESH,
        )

    def add_and_send(slot, flow, piece, step, incoming):
        cols = pl.ds(*spans[piece])
        total = mine[slot, :, cols].astype(f32) + pin[slot, :, cols].astype(f32)
        if incoming:
            sum_copy(slot, flow, piece, step - 1).wait_recv()
            total = total + rsin[flow, step - 1, :, cols].astype(f32)
        mine[slot, :, cols] = total.astype(bf16)
        sum_copy(slot, flow, piece, step).start()

    for flow in range(2):
        give(0, flow).wait_recv()
        for piece in range(PIECES):
            if side_of[piece] == flow:
                add_and_send(1, flow, piece, 0, False)
    for flow in range(2):
        give(last, flow).wait_recv()
    for incoming in (False, True):
        for piece in range(PIECES):
            flow = side_of[piece] if incoming else 1 - side_of[piece]
            add_and_send(2 * last + flow, flow, piece, 1, incoming)

    def fold(step, carry):
        s = half - step
        for side in range(2):
            give(s, side).wait_recv()
        for piece in range(PIECES):
            for flow in range(2):
                add_and_send(2 * s + flow, flow, piece, step, True)
        return carry

    lax.fori_loop(2, half, fold, 0)

    for piece in range(PIECES):
        cols = pl.ds(*spans[piece])
        total = resid_ref[:, cols] + mine[0, :, cols].astype(f32) + pin[0, :, cols].astype(f32)
        for flow in range(2):
            sum_copy(0, flow, piece, half - 1).wait_recv()
            total = total + rsin[flow, half - 1, :, cols].astype(f32)
        out_ref[:, cols] = total.astype(bf16)

    def drain_ring(s, carry):
        for flow in range(2):
            for piece in range(PIECES):
                ring_copy(x_ref, 1, flow, piece, s).wait_send()
        return carry

    lax.fori_loop(1, half, drain_ring, 0)
    for piece in range(PIECES):
        ring_copy(x_ref, 1, side_of[piece], piece, half).wait_send()

    def drain_slots(slot, carry):
        for piece in range(PIECES):
            partner_copy(x_ref, slot, piece).wait_send()
        return carry

    lax.fori_loop(0, ring, drain_slots, 0)

    def drain_groups(g, carry):
        for side in range(2):
            give(g, side).wait_send()
        return carry

    lax.fori_loop(0, half, drain_groups, 0)

    def drain_sums(step, carry):
        for flow in range(2):
            for piece in range(PIECES):
                sum_copy(0, flow, piece, step).wait_send()
        return carry

    for piece in range(PIECES):
        sum_copy(0, side_of[piece], piece, 0).wait_send()
    lax.fori_loop(1, half, drain_sums, 0)


def expert_layer(x_wide, resid, w_gate, w_up, w_down):
    ring = lax.axis_size("tok")
    half = ring // 2
    block, width = resid.shape
    ffs = w_gate.shape[1]
    wide = x_wide.shape[1]
    vmem = pl.BlockSpec(memory_space=pltpu.VMEM)
    hbm = pl.BlockSpec(memory_space=pltpu.HBM)
    dma = pltpu.SemaphoreType.DMA
    return pl.pallas_call(
        functools.partial(expert_kernel, half),
        out_shape=jax.ShapeDtypeStruct((block, width), bf16),
        in_specs=[vmem, vmem, hbm, hbm, hbm],
        out_specs=vmem,
        scratch_shapes=[
            pltpu.VMEM((ring, 2, block, wide), bf16),
            pltpu.VMEM((width, 2 * ffs), bf16),
            pltpu.VMEM((ffs, width), bf16),
            pltpu.VMEM((4 * block, 2 * ffs), f32),
            pltpu.VMEM((4 * block, ffs), bf16),
            pltpu.VMEM((ring, block, width), bf16),
            pltpu.VMEM((ring, block, width), bf16),
            pltpu.VMEM((ring, block, width), bf16),
            pltpu.VMEM((2, half, block, width), bf16),
            dma((3,)),
            dma((half + 1, 2, PIECES)),
            dma((half + 1, 2, PIECES)),
            dma((ring, PIECES)),
            dma((ring, PIECES)),
            dma((half, 2)),
            dma((half, 2)),
            dma((half, 2, PIECES)),
            dma((half, 2, PIECES)),
        ],
        compiler_params=pltpu.CompilerParams(
            collective_id=1, has_side_effects=True, vmem_limit_bytes=67043328
        ),
        name="expert_layer",
    )(x_wide, resid, w_gate, w_up, w_down)


def shards(
    hidden,
    queries,
    cache,
    cache_lengths,
    wkv,
    wo,
    attn_gain,
    moe_gain,
    w_gate,
    w_up,
    w_down,
    expert_ids,
    gates,
):
    x_wide, resid, fresh = prelude(
        hidden, queries, cache, cache_lengths, wkv, wo, attn_gain, moe_gain, expert_ids, gates
    )
    mixed = expert_layer(x_wide, resid, w_gate[0], w_up[0], w_down[0])
    fresh_key_value = fresh.reshape(fresh.shape[0], *wkv.shape[1:])
    return (mixed, fresh_key_value)


def solution(mesh):
    in_specs = (
        P(("grp", "tok"), "mdl"),
        P(("grp", "tok"), "mdl", None),
        P(("grp", "tok"), None, "mdl", None, None),
        P(("grp", "tok")),
        P("tok", "mdl", None, None),
        P("mdl", None, "tok"),
        P(),
        P(),
        P(("tok", "mdl"), None, None),
        P(("tok", "mdl"), None, None),
        P(("tok", "mdl"), None, None),
        P(("grp", "tok", "mdl"), None),
        P(("grp", "tok", "mdl"), None),
    )
    out_specs = (P(("grp", "tok", "mdl"), None), P(("grp", "tok"), "mdl", None, None))
    return jax.shard_map(shards, mesh=mesh, in_specs=in_specs, out_specs=out_specs, check_vma=False)
```

```python
import functools
import math

import jax
import jax.numpy as jnp
from jax import lax
from jax.experimental import pallas as pl
from jax.experimental.pallas import tpu as pltpu
from jax.sharding import PartitionSpec as P

EXPERTS = 4
TOPK = 2

eps_norm = 1e-05
rope_base = 1000000.0
mask_fill = -1e30

MESH = pl.DeviceIdType.MESH
bf16 = jnp.bfloat16
f32 = jnp.float32


LANES = 128
KEYS = 512


def permutation(groups, size):
    each = size // groups
    row = lax.broadcasted_iota(jnp.int32, (size, size), 0)
    col = lax.broadcasted_iota(jnp.int32, (size, size), 1)
    return jnp.where(col == lax.rem(row, each) * groups + row // each, 1.0, 0.0).astype(bf16)


def prelude_kernel(
    half,
    side,
    hid_ref,
    q_ref,
    cache_hbm,
    len_ref,
    wkv_ref,
    wo_ref,
    again_ref,
    mgain_ref,
    ids_ref,
    gates_ref,
    x_ref,
    resid_ref,
    fresh_ref,
    hfull,
    normed,
    kvbuf,
    wobuf,
    raw,
    keys,
    vals,
    qs,
    kvacc,
    smax,
    ssum,
    sacc,
    heads,
    part,
    part_in,
    csem,
    h_send,
    h_recv,
    kv_send,
    kv_recv,
    kvn_send,
    kvn_recv,
    wo_send,
    wo_recv,
    won_send,
    won_recv,
    p_send,
    p_recv,
):
    ring = 2 * half
    z = lax.axis_index("tok")
    m = lax.axis_index("mdl")
    gid = lax.axis_index("grp")
    ahead = lax.rem(z + 1, ring)
    behind = lax.rem(z + ring - 1, ring)
    odd_a = lax.rem(gid // side, 2)
    odd_b = lax.rem(gid, 2)
    neighbours = ({"grp": gid + side * (1 - 2 * odd_a)}, {"grp": gid + 1 - 2 * odd_b})
    own = 2 * odd_a + odd_b
    quarters = (own, 3 - own)
    partner = {"mdl": 1 - m}
    span, wide_half = hid_ref.shape
    block = span // 2
    width = resid_ref.shape[1]
    chip_cols = width // ring
    kv_heads = keys.shape[0]
    positions = keys.shape[1]
    head_total, _, head_dim = qs.shape
    per_group = head_total // kv_heads
    rows = per_group * span
    scale = 1.0 / math.sqrt(head_dim)

    load = pltpu.make_async_copy(cache_hbm, raw, csem.at[0])
    load.start()

    barrier = pltpu.get_barrier_semaphore()
    for who in ({"tok": ahead}, {"tok": behind}, *neighbours, partner):
        pl.semaphore_signal(barrier, inc=1, device_id=who, device_id_type=MESH)

    four = 2 * kv_heads
    perm4 = permutation(four, 64 * four)
    for q in range(4):
        got = jnp.dot(perm4, wkv_ref[q], preferred_element_type=f32).astype(bf16)
        for j in range(four):
            kvbuf[0, q, :, pl.ds(j * head_dim, head_dim)] = got[j * 64 : (j + 1) * 64]
    pl.semaphore_wait(barrier, 5)

    hid_copy = pltpu.make_async_remote_copy(
        src_ref=hid_ref,
        dst_ref=hfull.at[m],
        send_sem=h_send.at[0],
        recv_sem=h_recv.at[0],
        device_id=partner,
        device_id_type=MESH,
    )
    hid_copy.start()

    kinds = {
        "kv": (kvbuf, kv_send, kv_recv, kvn_send, kvn_recv),
        "wo": (wobuf, wo_send, wo_recv, won_send, won_recv),
    }

    def slot_of(step, flow):
        return 1 if isinstance(step, int) and step == half else 2 * step + flow

    def ring_copy(kind, src, step, flow, piece):
        buf, send, recv, _, _ = kinds[kind]
        q = quarters[piece]
        return pltpu.make_async_remote_copy(
            src_ref=src.at[q],
            dst_ref=buf.at[slot_of(step, flow), q],
            send_sem=send.at[step, flow, piece],
            recv_sem=recv.at[step, flow, piece],
            device_id={"tok": behind if flow == 0 else ahead},
            device_id_type=MESH,
        )

    def side_copy(kind, slot, axis):
        buf, _, _, send, recv = kinds[kind]
        return pltpu.make_async_remote_copy(
            src_ref=buf.at[slot, own],
            dst_ref=buf.at[slot, own],
            send_sem=send.at[slot, axis],
            recv_sem=recv.at[slot, axis],
            device_id=neighbours[axis],
            device_id_type=MESH,
        )

    def arrive(kind, step, pieces=(0, 1)):
        buf = kinds[kind][0]
        for piece in pieces:
            for flow in range(2):
                final = isinstance(step, int) and step == half
                if final and flow != piece:
                    continue
                slot = slot_of(step, flow)
                ring_copy(kind, buf.at[slot], step, flow, piece).wait_recv()
                if not final:
                    turn = isinstance(step, int) and step == half - 1
                    if not turn or flow == piece:
                        ring_copy(kind, buf.at[slot], step + 1, flow, piece).start()
                if piece == 0:
                    for axis in range(2):
                        side_copy(kind, slot, axis).start()

    def settle(kind, slot):
        for axis in range(2):
            side_copy(kind, slot, axis).wait_recv()

    for piece in range(2):
        for flow in range(2):
            ring_copy("kv", kvbuf.at[0], 1, flow, piece).start()
    for piece in range(2):
        for flow in range(2):
            ring_copy("wo", wo_ref, 1, flow, piece).start()

    lane = lax.broadcasted_iota(jnp.int32, (16, block), 0)
    route = jnp.zeros((16, block), f32)
    for k in range(TOPK):
        hit = (ids_ref[k : k + 1, :] == lane) | (ids_ref[k : k + 1, :] + EXPERTS == lane)
        route = route + jnp.where(hit, gates_ref[k : k + 1, :], 0.0)
    high = route.astype(bf16).astype(f32)
    terms = jnp.where(lane < EXPERTS, high, route - high)
    place = lax.broadcasted_iota(jnp.int32, (16, LANES), 0) == lax.broadcasted_iota(
        jnp.int32, (16, LANES), 1
    )
    tail = lax.dot_general(
        terms.astype(bf16),
        jnp.where(place, 1.0, 0.0).astype(bf16),
        (((0,), (0,)), ((), ())),
        preferred_element_type=f32,
    )
    x_ref[:, pl.ds(width, LANES)] = tail.astype(bf16)

    perm_q = permutation(head_total, 32 * head_total)
    for b in range(span // 32):
        got = jnp.dot(perm_q, q_ref[b], preferred_element_type=f32).astype(bf16)
        for h in range(head_total):
            qs[h, pl.ds(32 * b, 32), :] = got[32 * h : 32 * (h + 1)]

    def gain_of(ref, c):
        each = chip_cols // LANES
        gains = [ref[c * each + j : c * each + j + 1, :].astype(f32) for j in range(each)]
        return jnp.concatenate(gains, axis=1)

    hfull[m] = hid_ref[...]
    hid_copy.wait_recv()
    square = jnp.zeros((span, LANES), f32)
    for j in range(width // LANES):
        v = hfull[j // (ring // 2 * chip_cols // LANES), :, pl.ds(j * LANES % wide_half, LANES)]
        v = v.astype(f32)
        square = square + v * v
    inv = lax.rsqrt(jnp.sum(square, axis=1, keepdims=True) / width + eps_norm)
    for c in range(ring):
        v = hfull[c * chip_cols // wide_half, :, pl.ds(c * chip_cols % wide_half, chip_cols)]
        gain = gain_of(again_ref, c)
        normed[c] = (v.astype(f32) * inv * gain).astype(bf16)

    def chip_of(slot):
        if isinstance(slot, int) and slot < 2:
            return lax.rem(z + slot * half, ring)
        step, flow = slot // 2, lax.rem(slot, 2)
        return lax.rem(z + ring + step * (1 - 2 * flow), ring)

    def kv_use(slot):
        weights = kvbuf[slot].reshape(chip_cols, four * head_dim)
        kvacc[...] += jnp.dot(normed[chip_of(slot)], weights, preferred_element_type=f32)

    kvacc[...] = jnp.zeros_like(kvacc)
    kv_use(0)

    load.wait()

    def unpack(b, carry):
        got = jnp.dot(
            perm4,
            raw[pl.ds(pl.multiple_of(b * 64 * four, 64 * four), 64 * four), :],
            preferred_element_type=f32,
        ).astype(bf16)
        at = pl.ds(pl.multiple_of(b * 64, 64), 64)
        for g in range(kv_heads):
            keys[g, at, :] = got[(2 * g) * 64 : (2 * g + 1) * 64]
            vals[g, at, :] = got[(2 * g + 1) * 64 : (2 * g + 2) * 64]
        return carry

    lax.fori_loop(0, positions // 64, unpack, 0)

    length = len_ref[0]
    smax[...] = jnp.full_like(smax, mask_fill)
    ssum[...] = jnp.zeros_like(ssum)
    sacc[...] = jnp.zeros_like(sacc)

    def attend(g, key_rows, value_rows, allowed):
        query_rows = qs[pl.ds(per_group * g, per_group)].reshape(rows, head_dim)
        scores = lax.dot_general(
            query_rows, key_rows, (((1,), (1,)), ((), ())), preferred_element_type=f32
        )
        scores = jnp.where(allowed, scores * scale, mask_fill)
        old = smax[g][:, :1]
        top = jnp.maximum(old, jnp.max(scores, axis=1, keepdims=True))
        weights = jnp.where(allowed, jnp.exp(scores - top), 0.0)
        fade = jnp.exp(old - top)
        smax[g] = jnp.broadcast_to(top, (rows, LANES))
        ssum[g] = ssum[g] * fade + jnp.sum(weights, axis=1, keepdims=True)
        sacc[g] = sacc[g] * fade + jnp.dot(
            weights.astype(bf16), value_rows, preferred_element_type=f32
        )

    key_blocks = positions // KEYS

    def cached(i):
        g = i // key_blocks
        lo = lax.rem(i, key_blocks) * KEYS
        if not isinstance(lo, int):
            lo = pl.multiple_of(lo, KEYS)
        col = lo + lax.broadcasted_iota(jnp.int32, (rows, KEYS), 1)
        attend(g, keys[g, pl.ds(lo, KEYS), :], vals[g, pl.ds(lo, KEYS), :], col < length)

    def kv_step(step):
        arrive("kv", step)
        cached(step - 1)

    def kv_settled(step):
        for flow in range(2):
            settle("kv", slot_of(step, flow))
            kv_use(slot_of(step, flow))

    kv_step(1)
    arrive("wo", 1, (0,))

    def pair(k):
        kv_step(2 * k)
        arrive("wo", k, (1,))
        kv_settled(2 * k - 1)
        kv_step(2 * k + 1)
        arrive("wo", k + 1, (0,))
        kv_settled(2 * k)

    def pairs(k, carry):
        pair(k)
        return carry

    lax.fori_loop(1, half // 2 - 1, pairs, 0)
    pair(half // 2 - 1)
    arrive("kv", half)
    arrive("wo", half // 2, (1,))
    kv_settled(half - 1)
    cached(jnp.int32(half - 1))
    settle("kv", 1)
    kv_use(1)

    lanes = lax.broadcasted_iota(jnp.int32, (span, head_dim), 1)
    place_of = lax.broadcasted_iota(jnp.int32, (span, head_dim), 0) + length
    pair_of = lax.rem(lanes, head_dim // 2).astype(f32)
    angle = place_of.astype(f32) * jnp.exp(pair_of * (-2.0 * math.log(rope_base) / head_dim))
    cosine = jnp.cos(angle)
    sine = jnp.where(lanes < head_dim // 2, -jnp.sin(angle), jnp.sin(angle))
    token = lax.rem(lax.broadcasted_iota(jnp.int32, (rows, span), 0), span)
    causal = lax.broadcasted_iota(jnp.int32, (rows, span), 1) <= token
    for g in range(kv_heads):
        k_cols = pl.ds(2 * g * head_dim, head_dim)
        v_cols = pl.ds((2 * g + 1) * head_dim, head_dim)
        key = kvacc[:, k_cols]
        turned = pltpu.roll(key, head_dim // 2, 1)
        fresh_ref[:, k_cols] = (key * cosine + turned * sine).astype(bf16)
        fresh_ref[:, v_cols] = kvacc[:, v_cols].astype(bf16)
        attend(g, fresh_ref[:, k_cols], fresh_ref[:, v_cols], causal)
        done = (sacc[g] / ssum[g]).astype(bf16)
        for h in range(per_group):
            at = pl.ds((g * per_group + h) * head_dim, head_dim)
            heads[:, at] = done[h * span : (h + 1) * span]

    def wo_use(slot, buf):
        weights = buf.reshape(4 * wo_ref.shape[1], chip_cols)
        got = jnp.dot(heads[...], weights, preferred_element_type=f32)
        for core in range(2):
            part[core, slot] = got[core * block : (core + 1) * block]

    def part_copy(g):
        return pltpu.make_async_remote_copy(
            src_ref=part.at[1 - m, pl.ds(2 * g, 2)],
            dst_ref=part_in.at[pl.ds(2 * g, 2)],
            send_sem=p_send.at[g],
            recv_sem=p_recv.at[g],
            device_id=partner,
            device_id_type=MESH,
        )

    def wo_settled(step):
        for flow in range(2):
            slot = slot_of(step, flow)
            settle("wo", slot)
            wo_use(slot, wobuf[slot])
        part_copy(step).start()

    def assemble(slot):
        c = chip_of(slot)
        cols = pl.ds(pl.multiple_of(c * chip_cols, chip_cols), chip_cols)
        in_half = pl.ds(
            pl.multiple_of(lax.rem(c * chip_cols, wide_half), chip_cols), chip_cols
        )
        mine = hfull[c * chip_cols // wide_half, pl.ds(pl.multiple_of(m * block, block), block), in_half]
        resid_ref[:, cols] = mine.astype(f32) + part[m, slot] + part_in[slot]

    def gather_parts(step):
        part_copy(step).wait_recv()
        for flow in range(2):
            assemble(slot_of(step, flow))

    wo_use(0, wo_ref[...])

    def late(s, carry):
        arrive("wo", s)
        first = 2 * (s - half // 2) - 1
        wo_settled(first)
        wo_settled(first + 1)
        return carry

    lax.fori_loop(half // 2 + 1, half - 1, late, 0)
    arrive("wo", half - 1)
    wo_settled(half - 3)

    def early(step, carry):
        gather_parts(step)
        return carry

    lax.fori_loop(1, half - 3, early, 0)
    arrive("wo", half)
    wo_settled(half - 2)
    wo_settled(half - 1)
    lax.fori_loop(half - 3, half, early, 0)
    settle("wo", 1)
    wo_use(1, wobuf[1])
    part_copy(0).start()
    part_copy(0).wait_recv()
    assemble(0)
    assemble(1)

    square = jnp.zeros((block, LANES), f32)
    for j in range(width // LANES):
        v = resid_ref[:, pl.ds(j * LANES, LANES)]
        square = square + v * v
    inv = lax.rsqrt(jnp.sum(square, axis=1, keepdims=True) / width + eps_norm)
    for c in range(ring):
        cols = pl.ds(c * chip_cols, chip_cols)
        gain = gain_of(mgain_ref, c)
        x_ref[:, cols] = (resid_ref[:, cols] * inv * gain).astype(bf16)

    hid_copy.wait_send()

    def drain_ring(step, carry):
        for kind in ("kv", "wo"):
            for flow in range(2):
                for piece in range(2):
                    ring_copy(kind, kinds[kind][0].at[0], step, flow, piece).wait_send()
        return carry

    lax.fori_loop(1, half, drain_ring, 0)
    for kind in ("kv", "wo"):
        for flow in range(2):
            ring_copy(kind, kinds[kind][0].at[0], half, flow, flow).wait_send()

    def drain_sides(slot, carry):
        for kind in ("kv", "wo"):
            for axis in range(2):
                side_copy(kind, slot, axis).wait_send()
        return carry

    lax.fori_loop(1, ring, drain_sides, 0)

    def drain_parts(g, carry):
        part_copy(g).wait_send()
        return carry

    lax.fori_loop(0, half, drain_parts, 0)


def prelude(hidden, queries, cache, cache_lengths, wkv, wo, attn_gain, moe_gain, expert_ids, gates):
    ring = lax.axis_size("tok")
    half = ring // 2
    side = math.isqrt(lax.axis_size("grp"))
    span, wide_half = hidden.shape
    block, width = span // 2, 2 * wide_half
    heads, head_dim = queries.shape[1:]
    positions, kv_heads = cache.shape[1:3]
    four = 2 * kv_heads
    chip_cols = width // ring
    rows = heads // kv_heads * span
    vmem = pl.BlockSpec(memory_space=pltpu.VMEM)
    hbm = pl.BlockSpec(memory_space=pltpu.HBM)
    smem = pl.BlockSpec(memory_space=pltpu.SMEM)
    dma = pltpu.SemaphoreType.DMA
    depth = heads * head_dim // 4
    return pl.pallas_call(
        functools.partial(prelude_kernel, half, side),
        out_shape=(
            jax.ShapeDtypeStruct((block, width + LANES), bf16),
            jax.ShapeDtypeStruct((block, width), f32),
            jax.ShapeDtypeStruct((span, four * head_dim), bf16),
        ),
        in_specs=[vmem, vmem, hbm, smem, vmem, vmem, vmem, vmem, vmem, vmem],
        out_specs=(vmem, vmem, vmem),
        scratch_shapes=[
            pltpu.VMEM((2, span, wide_half), bf16),
            pltpu.VMEM((ring, span, chip_cols), bf16),
            pltpu.VMEM((ring, 4, chip_cols // 4, four * head_dim), bf16),
            pltpu.VMEM((ring, 4, depth, chip_cols), bf16),
            pltpu.VMEM((positions * four, head_dim), bf16),
            pltpu.VMEM((kv_heads, positions, head_dim), bf16),
            pltpu.VMEM((kv_heads, positions, head_dim), bf16),
            pltpu.VMEM((heads, span, head_dim), bf16),
            pltpu.VMEM((span, four * head_dim), f32),
            pltpu.VMEM((kv_heads, rows, LANES), f32),
            pltpu.VMEM((kv_heads, rows, LANES), f32),
            pltpu.VMEM((kv_heads, rows, head_dim), f32),
            pltpu.VMEM((span, heads * head_dim), bf16),
            pltpu.VMEM((2, ring, block, chip_cols), f32),
            pltpu.VMEM((ring, block, chip_cols), f32),
            dma((1,)),
            dma((1,)),
            dma((1,)),
            dma((half + 1, 2, 2)),
            dma((half + 1, 2, 2)),
            dma((ring, 2)),
            dma((ring, 2)),
            dma((half + 1, 2, 2)),
            dma((half + 1, 2, 2)),
            dma((ring, 2)),
            dma((ring, 2)),
            dma((half,)),
            dma((half,)),
        ],
        compiler_params=pltpu.CompilerParams(
            collective_id=0, has_side_effects=True, vmem_limit_bytes=67043328
        ),
        name="prelude",
    )(
        hidden,
        queries.reshape(span // 32, 32 * heads, head_dim),
        cache.reshape(positions * four, head_dim),
        cache_lengths,
        wkv.reshape(4, chip_cols // 4 * four, head_dim),
        wo.reshape(4, depth, chip_cols),
        attn_gain.reshape(width // LANES, LANES),
        moe_gain.reshape(width // LANES, LANES),
        expert_ids.T,
        gates.T,
    )


PIECES = 2


def expert_kernel(
    half,
    x_ref,
    resid_ref,
    wg_hbm,
    wu_hbm,
    wd_hbm,
    out_ref,
    xs,
    wgu,
    wd,
    gu,
    hid,
    mine,
    pout,
    pin,
    rsin,
    wsem,
    ag_send,
    ag_recv,
    x_send,
    x_recv,
    p_send,
    p_recv,
    rs_send,
    rs_recv,
):
    ring = 2 * half
    z = lax.axis_index("tok")
    m = lax.axis_index("mdl")
    ahead = lax.rem(z + 1, ring)
    behind = lax.rem(z + ring - 1, ring)
    partner = {"mdl": 1 - m}
    expert = z // (ring // EXPERTS)
    block, width = resid_ref.shape
    ffs = wg_hbm.shape[1]
    cut = width // PIECES
    spans = [(i * cut, cut) for i in range(PIECES)]
    wide_spans = spans[:-1] + [(width - cut, cut + LANES)]
    side_of = [i * 2 // PIECES for i in range(PIECES)]

    loads = (
        pltpu.make_async_copy(wg_hbm, wgu.at[:, pl.ds(0, ffs)], wsem.at[0]),
        pltpu.make_async_copy(wu_hbm, wgu.at[:, pl.ds(ffs, ffs)], wsem.at[1]),
        pltpu.make_async_copy(wd_hbm, wd, wsem.at[2]),
    )

    barrier = pltpu.get_barrier_semaphore()
    for who in ({"tok": ahead}, {"tok": behind}, partner):
        pl.semaphore_signal(barrier, inc=1, device_id=who, device_id_type=MESH)
    pl.semaphore_wait(barrier, 3)

    def ring_copy(src, dst_slot, flow, piece, step):
        cols = pl.ds(*wide_spans[piece])
        return pltpu.make_async_remote_copy(
            src_ref=src.at[:, cols],
            dst_ref=xs.at[dst_slot, 0, :, cols],
            send_sem=ag_send.at[step, flow, piece],
            recv_sem=ag_recv.at[step, flow, piece],
            device_id={"tok": behind if flow == 0 else ahead},
            device_id_type=MESH,
        )

    def partner_copy(src, slot, piece):
        cols = pl.ds(*wide_spans[piece])
        return pltpu.make_async_remote_copy(
            src_ref=src.at[:, cols],
            dst_ref=xs.at[slot, 1, :, cols],
            send_sem=x_send.at[slot, piece],
            recv_sem=x_recv.at[slot, piece],
            device_id=partner,
            device_id_type=MESH,
        )

    for piece in range(PIECES):
        for flow in range(2):
            ring_copy(x_ref, 2 + flow, flow, piece, 1).start()
    for load in loads:
        load.start()
    for piece in range(PIECES):
        partner_copy(x_ref, 0, piece).start()
    xs[0, 0] = x_ref[...]

    def gate_up(g):
        rows = xs[pl.ds(2 * g, 2), :, :, pl.ds(0, width)].reshape(4 * block, width)
        gu[...] = jnp.dot(rows, wgu[...], preferred_element_type=f32)

    def activate():
        gate = gu[:, pl.ds(0, ffs)]
        up = gu[:, pl.ds(ffs, ffs)]
        hid[...] = (gate / (1.0 + jnp.exp(-gate)) * up).astype(bf16)

    def weight_of(g):
        tail = xs[pl.ds(2 * g, 2), :, :, pl.ds(width, LANES)].reshape(4 * block, LANES)
        lane = lax.broadcasted_iota(jnp.int32, (4 * block, LANES), 1)
        pick = (lane == expert) | (lane == expert + EXPERTS)
        return jnp.sum(jnp.where(pick, tail.astype(f32), 0.0), axis=1, keepdims=True)

    def down(g, side):
        weight = weight_of(g)
        cols = pl.ds(side * (width // 2), width // 2)
        got = jnp.dot(hid[...], wd[:, cols], preferred_element_type=f32) * weight
        got = got.astype(bf16)
        for slot in range(2):
            mine[2 * g + slot, :, cols] = got[2 * slot * block : (2 * slot + 1) * block]
            pout[2 * g + slot, :, cols] = got[(2 * slot + 1) * block : (2 * slot + 2) * block]

    def give(g, side):
        cols = pl.ds(side * (width // 2), width // 2)
        return pltpu.make_async_remote_copy(
            src_ref=pout.at[pl.ds(2 * g, 2), :, cols],
            dst_ref=pin.at[pl.ds(2 * g, 2), :, cols],
            send_sem=p_send.at[g, side],
            recv_sem=p_recv.at[g, side],
            device_id=partner,
            device_id_type=MESH,
        )

    def await_partner(g):
        for slot in range(2):
            for piece in range(PIECES):
                partner_copy(x_ref, 2 * g + slot, piece).wait_recv()

    def arrive(s, flow, piece, onward):
        ring_copy(x_ref, 2 * s + flow, flow, piece, s).wait_recv()
        if onward is not None:
            ring_copy(xs.at[2 * s + flow, 0], onward, flow, piece, s + 1).start()
        partner_copy(xs.at[2 * s + flow, 0], 2 * s + flow, piece).start()

    for piece in range(PIECES):
        for flow in range(2):
            arrive(1, flow, piece, 4 + flow)
        if piece == 0:
            for load in loads:
                load.wait()

    last = half - 1

    def events(s, piece):
        @pl.when(s < last)
        def _():
            for flow in range(2):
                arrive(s, flow, piece, 2 * (s + 1) + flow)

        @pl.when(s == last)
        def _():
            for flow in range(2):
                arrive(last, flow, piece, 1 if flow == side_of[piece] else None)

        @pl.when(s == half)
        def _():
            ring_copy(x_ref, 1, side_of[piece], piece, half).wait_recv()
            partner_copy(xs.at[1, 0], 1, piece).start()

    def body(s, carry):
        g = lax.rem(s - 1, half)
        for piece in range(PIECES // 2):
            events(s, piece)
        await_partner(g)
        gate_up(g)
        for piece in range(PIECES // 2, PIECES):
            events(s, piece)
        activate()
        for side in range(2):
            down(g, side)
            give(g, side).start()
        return carry

    lax.fori_loop(2, half + 2, body, 0)

    def sum_copy(slot, flow, piece, step):
        cols = pl.ds(*spans[piece])
        return pltpu.make_async_remote_copy(
            src_ref=mine.at[slot, :, cols],
            dst_ref=rsin.at[flow, step, :, cols],
            send_sem=rs_send.at[step, flow, piece],
            recv_sem=rs_recv.at[step, flow, piece],
            device_id={"tok": ahead if flow == 0 else behind},
            device_id_type=MESH,
        )

    def add_and_send(slot, flow, piece, step, incoming):
        cols = pl.ds(*spans[piece])
        total = mine[slot, :, cols].astype(f32) + pin[slot, :, cols].astype(f32)
        if incoming:
            sum_copy(slot, flow, piece, step - 1).wait_recv()
            total = total + rsin[flow, step - 1, :, cols].astype(f32)
        mine[slot, :, cols] = total.astype(bf16)
        sum_copy(slot, flow, piece, step).start()

    for flow in range(2):
        give(0, flow).wait_recv()
        for piece in range(PIECES):
            if side_of[piece] == flow:
                add_and_send(1, flow, piece, 0, False)
    for flow in range(2):
        give(last, flow).wait_recv()
    for incoming in (False, True):
        for piece in range(PIECES):
            flow = side_of[piece] if incoming else 1 - side_of[piece]
            add_and_send(2 * last + flow, flow, piece, 1, incoming)

    def fold(step, carry):
        s = half - step
        for side in range(2):
            give(s, side).wait_recv()
        for piece in range(PIECES):
            for flow in range(2):
                add_and_send(2 * s + flow, flow, piece, step, True)
        return carry

    lax.fori_loop(2, half, fold, 0)

    for piece in range(PIECES):
        cols = pl.ds(*spans[piece])
        total = resid_ref[:, cols] + mine[0, :, cols].astype(f32) + pin[0, :, cols].astype(f32)
        for flow in range(2):
            sum_copy(0, flow, piece, half - 1).wait_recv()
            total = total + rsin[flow, half - 1, :, cols].astype(f32)
        out_ref[:, cols] = total.astype(bf16)

    def drain_ring(s, carry):
        for flow in range(2):
            for piece in range(PIECES):
                ring_copy(x_ref, 1, flow, piece, s).wait_send()
        return carry

    lax.fori_loop(1, half, drain_ring, 0)
    for piece in range(PIECES):
        ring_copy(x_ref, 1, side_of[piece], piece, half).wait_send()

    def drain_slots(slot, carry):
        for piece in range(PIECES):
            partner_copy(x_ref, slot, piece).wait_send()
        return carry

    lax.fori_loop(0, ring, drain_slots, 0)

    def drain_groups(g, carry):
        for side in range(2):
            give(g, side).wait_send()
        return carry

    lax.fori_loop(0, half, drain_groups, 0)

    def drain_sums(step, carry):
        for flow in range(2):
            for piece in range(PIECES):
                sum_copy(0, flow, piece, step).wait_send()
        return carry

    for piece in range(PIECES):
        sum_copy(0, side_of[piece], piece, 0).wait_send()
    lax.fori_loop(1, half, drain_sums, 0)


def expert_layer(x_wide, resid, w_gate, w_up, w_down):
    ring = lax.axis_size("tok")
    half = ring // 2
    block, width = resid.shape
    ffs = w_gate.shape[1]
    wide = x_wide.shape[1]
    vmem = pl.BlockSpec(memory_space=pltpu.VMEM)
    hbm = pl.BlockSpec(memory_space=pltpu.HBM)
    dma = pltpu.SemaphoreType.DMA
    return pl.pallas_call(
        functools.partial(expert_kernel, half),
        out_shape=jax.ShapeDtypeStruct((block, width), bf16),
        in_specs=[vmem, vmem, hbm, hbm, hbm],
        out_specs=vmem,
        scratch_shapes=[
            pltpu.VMEM((ring, 2, block, wide), bf16),
            pltpu.VMEM((width, 2 * ffs), bf16),
            pltpu.VMEM((ffs, width), bf16),
            pltpu.VMEM((4 * block, 2 * ffs), f32),
            pltpu.VMEM((4 * block, ffs), bf16),
            pltpu.VMEM((ring, block, width), bf16),
            pltpu.VMEM((ring, block, width), bf16),
            pltpu.VMEM((ring, block, width), bf16),
            pltpu.VMEM((2, half, block, width), bf16),
            dma((3,)),
            dma((half + 1, 2, PIECES)),
            dma((half + 1, 2, PIECES)),
            dma((ring, PIECES)),
            dma((ring, PIECES)),
            dma((half, 2)),
            dma((half, 2)),
            dma((half, 2, PIECES)),
            dma((half, 2, PIECES)),
        ],
        compiler_params=pltpu.CompilerParams(
            collective_id=1, has_side_effects=True, vmem_limit_bytes=67043328
        ),
        name="expert_layer",
    )(x_wide, resid, w_gate, w_up, w_down)


def shards(
    hidden,
    queries,
    cache,
    cache_lengths,
    wkv,
    wo,
    attn_gain,
    moe_gain,
    w_gate,
    w_up,
    w_down,
    expert_ids,
    gates,
):
    x_wide, resid, fresh = prelude(
        hidden, queries, cache, cache_lengths, wkv, wo, attn_gain, moe_gain, expert_ids, gates
    )
    mixed = expert_layer(x_wide, resid, w_gate[0], w_up[0], w_down[0])
    fresh_key_value = fresh.reshape(fresh.shape[0], *wkv.shape[1:])
    return (mixed, fresh_key_value)


def solution(mesh):
    in_specs = (
        P(("grp", "tok"), "mdl"),
        P(("grp", "tok"), "mdl", None),
        P(("grp", "tok"), None, "mdl", None, None),
        P(("grp", "tok")),
        P("tok", "mdl", None, None),
        P("mdl", None, "tok"),
        P(),
        P(),
        P(("tok", "mdl"), None, None),
        P(("tok", "mdl"), None, None),
        P(("tok", "mdl"), None, None),
        P(("grp", "tok", "mdl"), None),
        P(("grp", "tok", "mdl"), None),
    )
    out_specs = (P(("grp", "tok", "mdl"), None), P(("grp", "tok"), "mdl", None, None))
    return jax.shard_map(shards, mesh=mesh, in_specs=in_specs, out_specs=out_specs, check_vma=False)
```

```python
import functools
import math

import jax
import jax.numpy as jnp
from jax import lax
from jax.experimental import pallas as pl
from jax.experimental.pallas import tpu as pltpu
from jax.sharding import PartitionSpec as P

EXPERTS = 4
TOPK = 2

eps_norm = 1e-05
rope_base = 1000000.0
mask_fill = -1e30

MESH = pl.DeviceIdType.MESH
bf16 = jnp.bfloat16
f32 = jnp.float32


LANES = 128
KEYS = 512


def permutation(groups, size):
    each = size // groups
    row = lax.broadcasted_iota(jnp.int32, (size, size), 0)
    col = lax.broadcasted_iota(jnp.int32, (size, size), 1)
    return jnp.where(col == lax.rem(row, each) * groups + row // each, 1.0, 0.0).astype(bf16)


def prelude_kernel(
    half,
    side,
    hid_ref,
    q_ref,
    cache_hbm,
    len_ref,
    wkv_ref,
    wo_ref,
    again_ref,
    mgain_ref,
    ids_ref,
    gates_ref,
    x_ref,
    resid_ref,
    rows_ref,
    fresh_ref,
    hfull,
    normed,
    kvbuf,
    wobuf,
    raw,
    keys,
    vals,
    qs,
    kvacc,
    smax,
    ssum,
    sacc,
    heads,
    part,
    part_in,
    csem,
    h_send,
    h_recv,
    kv_send,
    kv_recv,
    kvn_send,
    kvn_recv,
    wo_send,
    wo_recv,
    won_send,
    won_recv,
    p_send,
    p_recv,
):
    ring = 2 * half
    z = lax.axis_index("tok")
    m = lax.axis_index("mdl")
    gid = lax.axis_index("grp")
    ahead = lax.rem(z + 1, ring)
    behind = lax.rem(z + ring - 1, ring)
    odd_a = lax.rem(gid // side, 2)
    odd_b = lax.rem(gid, 2)
    neighbours = ({"grp": gid + side * (1 - 2 * odd_a)}, {"grp": gid + 1 - 2 * odd_b})
    own = 2 * odd_a + odd_b
    quarters = (own, 3 - own)
    partner = {"mdl": 1 - m}
    span, wide_half = hid_ref.shape
    block = span // 2
    width = resid_ref.shape[1]
    chip_cols = width // ring
    kv_heads = keys.shape[0]
    positions = keys.shape[1]
    head_total, _, head_dim = qs.shape
    per_group = head_total // kv_heads
    rows = per_group * span
    scale = 1.0 / math.sqrt(head_dim)

    load = pltpu.make_async_copy(cache_hbm, raw, csem.at[0])
    load.start()

    barrier = pltpu.get_barrier_semaphore()
    for who in ({"tok": ahead}, {"tok": behind}, *neighbours, partner):
        pl.semaphore_signal(barrier, inc=1, device_id=who, device_id_type=MESH)

    four = 2 * kv_heads
    perm4 = permutation(four, 64 * four)
    for q in range(4):
        got = jnp.dot(perm4, wkv_ref[q], preferred_element_type=f32).astype(bf16)
        for j in range(four):
            kvbuf[0, q, :, pl.ds(j * head_dim, head_dim)] = got[j * 64 : (j + 1) * 64]
    pl.semaphore_wait(barrier, 5)

    hid_copy = pltpu.make_async_remote_copy(
        src_ref=hid_ref,
        dst_ref=hfull.at[m],
        send_sem=h_send.at[0],
        recv_sem=h_recv.at[0],
        device_id=partner,
        device_id_type=MESH,
    )
    hid_copy.start()

    kinds = {
        "kv": (kvbuf, kv_send, kv_recv, kvn_send, kvn_recv),
        "wo": (wobuf, wo_send, wo_recv, won_send, won_recv),
    }

    def slot_of(step, flow):
        return 1 if isinstance(step, int) and step == half else 2 * step + flow

    def ring_copy(kind, src, step, flow, piece):
        buf, send, recv, _, _ = kinds[kind]
        q = quarters[piece]
        return pltpu.make_async_remote_copy(
            src_ref=src.at[q],
            dst_ref=buf.at[slot_of(step, flow), q],
            send_sem=send.at[step, flow, piece],
            recv_sem=recv.at[step, flow, piece],
            device_id={"tok": behind if flow == 0 else ahead},
            device_id_type=MESH,
        )

    def side_copy(kind, slot, axis):
        buf, _, _, send, recv = kinds[kind]
        return pltpu.make_async_remote_copy(
            src_ref=buf.at[slot, own],
            dst_ref=buf.at[slot, own],
            send_sem=send.at[slot, axis],
            recv_sem=recv.at[slot, axis],
            device_id=neighbours[axis],
            device_id_type=MESH,
        )

    def arrive(kind, step, pieces=(0, 1)):
        buf = kinds[kind][0]
        for piece in pieces:
            for flow in range(2):
                final = isinstance(step, int) and step == half
                if final and flow != piece:
                    continue
                slot = slot_of(step, flow)
                ring_copy(kind, buf.at[slot], step, flow, piece).wait_recv()
                if not final:
                    turn = isinstance(step, int) and step == half - 1
                    if not turn or flow == piece:
                        ring_copy(kind, buf.at[slot], step + 1, flow, piece).start()
                if piece == 0:
                    for axis in range(2):
                        side_copy(kind, slot, axis).start()

    def settle(kind, slot):
        for axis in range(2):
            side_copy(kind, slot, axis).wait_recv()

    for piece in range(2):
        for flow in range(2):
            ring_copy("kv", kvbuf.at[0], 1, flow, piece).start()
    for piece in range(2):
        for flow in range(2):
            ring_copy("wo", wo_ref, 1, flow, piece).start()

    lane = lax.broadcasted_iota(jnp.int32, (16, block), 0)
    route = jnp.zeros((16, block), f32)
    for k in range(TOPK):
        hit = (ids_ref[k : k + 1, :] == lane) | (ids_ref[k : k + 1, :] + EXPERTS == lane)
        route = route + jnp.where(hit, gates_ref[k : k + 1, :], 0.0)
    high = route.astype(bf16).astype(f32)
    terms = jnp.where(lane < EXPERTS, high, route - high)
    place = lax.broadcasted_iota(jnp.int32, (16, LANES), 0) == lax.broadcasted_iota(
        jnp.int32, (16, LANES), 1
    )
    tail = lax.dot_general(
        terms.astype(bf16),
        jnp.where(place, 1.0, 0.0).astype(bf16),
        (((0,), (0,)), ((), ())),
        preferred_element_type=f32,
    )
    x_ref[:, pl.ds(width, LANES)] = tail.astype(bf16)

    perm_q = permutation(head_total, 32 * head_total)
    for b in range(span // 32):
        got = jnp.dot(perm_q, q_ref[b], preferred_element_type=f32).astype(bf16)
        for h in range(head_total):
            qs[h, pl.ds(32 * b, 32), :] = got[32 * h : 32 * (h + 1)]

    def gain_of(ref, c):
        each = chip_cols // LANES
        gains = [ref[c * each + j : c * each + j + 1, :].astype(f32) for j in range(each)]
        return jnp.concatenate(gains, axis=1)

    hfull[m] = hid_ref[...]
    hid_copy.wait_recv()
    square = jnp.zeros((span, LANES), f32)
    for j in range(width // LANES):
        v = hfull[j // (ring // 2 * chip_cols // LANES), :, pl.ds(j * LANES % wide_half, LANES)]
        v = v.astype(f32)
        square = square + v * v
    inv = lax.rsqrt(jnp.sum(square, axis=1, keepdims=True) / width + eps_norm)
    for c in range(ring):
        v = hfull[c * chip_cols // wide_half, :, pl.ds(c * chip_cols % wide_half, chip_cols)]
        gain = gain_of(again_ref, c)
        normed[c] = (v.astype(f32) * inv * gain).astype(bf16)

    def chip_of(slot):
        if isinstance(slot, int) and slot < 2:
            return lax.rem(z + slot * half, ring)
        step, flow = slot // 2, lax.rem(slot, 2)
        return lax.rem(z + ring + step * (1 - 2 * flow), ring)

    def kv_use(slot):
        weights = kvbuf[slot].reshape(chip_cols, four * head_dim)
        kvacc[...] += jnp.dot(normed[chip_of(slot)], weights, preferred_element_type=f32)

    kvacc[...] = jnp.zeros_like(kvacc)
    kv_use(0)

    load.wait()

    def unpack(b, carry):
        got = jnp.dot(
            perm4,
            raw[pl.ds(pl.multiple_of(b * 64 * four, 64 * four), 64 * four), :],
            preferred_element_type=f32,
        ).astype(bf16)
        at = pl.ds(pl.multiple_of(b * 64, 64), 64)
        for g in range(kv_heads):
            keys[g, at, :] = got[(2 * g) * 64 : (2 * g + 1) * 64]
            vals[g, at, :] = got[(2 * g + 1) * 64 : (2 * g + 2) * 64]
        return carry

    lax.fori_loop(0, positions // 64, unpack, 0)

    length = len_ref[0]
    smax[...] = jnp.full_like(smax, mask_fill)
    ssum[...] = jnp.zeros_like(ssum)
    sacc[...] = jnp.zeros_like(sacc)

    def attend(g, key_rows, value_rows, allowed):
        query_rows = qs[pl.ds(per_group * g, per_group)].reshape(rows, head_dim)
        scores = lax.dot_general(
            query_rows, key_rows, (((1,), (1,)), ((), ())), preferred_element_type=f32
        )
        scores = jnp.where(allowed, scores * scale, mask_fill)
        old = smax[g][:, :1]
        top = jnp.maximum(old, jnp.max(scores, axis=1, keepdims=True))
        weights = jnp.where(allowed, jnp.exp(scores - top), 0.0)
        fade = jnp.exp(old - top)
        smax[g] = jnp.broadcast_to(top, (rows, LANES))
        ssum[g] = ssum[g] * fade + jnp.sum(weights, axis=1, keepdims=True)
        sacc[g] = sacc[g] * fade + jnp.dot(
            weights.astype(bf16), value_rows, preferred_element_type=f32
        )

    key_blocks = positions // KEYS

    def cached(i):
        g = i // key_blocks
        lo = lax.rem(i, key_blocks) * KEYS
        if not isinstance(lo, int):
            lo = pl.multiple_of(lo, KEYS)
        col = lo + lax.broadcasted_iota(jnp.int32, (rows, KEYS), 1)
        attend(g, keys[g, pl.ds(lo, KEYS), :], vals[g, pl.ds(lo, KEYS), :], col < length)

    def kv_step(step):
        arrive("kv", step)
        cached(step - 1)

    def kv_settled(step):
        for flow in range(2):
            settle("kv", slot_of(step, flow))
            kv_use(slot_of(step, flow))

    kv_step(1)
    arrive("wo", 1, (0,))

    def pair(k):
        kv_step(2 * k)
        arrive("wo", k, (1,))
        kv_settled(2 * k - 1)
        kv_step(2 * k + 1)
        arrive("wo", k + 1, (0,))
        kv_settled(2 * k)

    def pairs(k, carry):
        pair(k)
        return carry

    lax.fori_loop(1, half // 2 - 1, pairs, 0)
    pair(half // 2 - 1)
    arrive("kv", half)
    arrive("wo", half // 2, (1,))
    kv_settled(half - 1)
    cached(jnp.int32(half - 1))
    settle("kv", 1)
    kv_use(1)

    lanes = lax.broadcasted_iota(jnp.int32, (span, head_dim), 1)
    place_of = lax.broadcasted_iota(jnp.int32, (span, head_dim), 0) + length
    pair_of = lax.rem(lanes, head_dim // 2).astype(f32)
    angle = place_of.astype(f32) * jnp.exp(pair_of * (-2.0 * math.log(rope_base) / head_dim))
    cosine = jnp.cos(angle)
    sine = jnp.where(lanes < head_dim // 2, -jnp.sin(angle), jnp.sin(angle))
    token = lax.rem(lax.broadcasted_iota(jnp.int32, (rows, span), 0), span)
    causal = lax.broadcasted_iota(jnp.int32, (rows, span), 1) <= token
    for g in range(kv_heads):
        k_cols = pl.ds(2 * g * head_dim, head_dim)
        v_cols = pl.ds((2 * g + 1) * head_dim, head_dim)
        key = kvacc[:, k_cols]
        turned = pltpu.roll(key, head_dim // 2, 1)
        fresh_ref[:, k_cols] = (key * cosine + turned * sine).astype(bf16)
        fresh_ref[:, v_cols] = kvacc[:, v_cols].astype(bf16)
        attend(g, fresh_ref[:, k_cols], fresh_ref[:, v_cols], causal)
        done = (sacc[g] / ssum[g]).astype(bf16)
        for h in range(per_group):
            at = pl.ds((g * per_group + h) * head_dim, head_dim)
            heads[:, at] = done[h * span : (h + 1) * span]

    columns = [fresh_ref[:, pl.ds(j * head_dim, head_dim)] for j in range(four)]
    rows_ref[...] = lax.dot_general(
        perm4,
        jnp.concatenate(columns, axis=0),
        (((0,), (0,)), ((), ())),
        preferred_element_type=f32,
    ).astype(bf16)

    def wo_use(slot, buf):
        weights = buf.reshape(4 * wo_ref.shape[1], chip_cols)
        got = jnp.dot(heads[...], weights, preferred_element_type=f32)
        for core in range(2):
            part[core, slot] = got[core * block : (core + 1) * block]

    def part_copy(g):
        return pltpu.make_async_remote_copy(
            src_ref=part.at[1 - m, pl.ds(2 * g, 2)],
            dst_ref=part_in.at[pl.ds(2 * g, 2)],
            send_sem=p_send.at[g],
            recv_sem=p_recv.at[g],
            device_id=partner,
            device_id_type=MESH,
        )

    def wo_settled(step):
        for flow in range(2):
            slot = slot_of(step, flow)
            settle("wo", slot)
            wo_use(slot, wobuf[slot])
        part_copy(step).start()

    def assemble(slot):
        c = chip_of(slot)
        cols = pl.ds(pl.multiple_of(c * chip_cols, chip_cols), chip_cols)
        in_half = pl.ds(
            pl.multiple_of(lax.rem(c * chip_cols, wide_half), chip_cols), chip_cols
        )
        mine = hfull[c * chip_cols // wide_half, pl.ds(pl.multiple_of(m * block, block), block), in_half]
        resid_ref[:, cols] = mine.astype(f32) + part[m, slot] + part_in[slot]

    def gather_parts(step):
        part_copy(step).wait_recv()
        for flow in range(2):
            assemble(slot_of(step, flow))

    wo_use(0, wo_ref[...])

    def late(s, carry):
        arrive("wo", s)
        first = 2 * (s - half // 2) - 1
        wo_settled(first)
        wo_settled(first + 1)
        return carry

    lax.fori_loop(half // 2 + 1, half - 1, late, 0)
    arrive("wo", half - 1)
    wo_settled(half - 3)

    def early(step, carry):
        gather_parts(step)
        return carry

    lax.fori_loop(1, half - 3, early, 0)
    arrive("wo", half)
    wo_settled(half - 2)
    wo_settled(half - 1)
    lax.fori_loop(half - 3, half, early, 0)
    settle("wo", 1)
    wo_use(1, wobuf[1])
    part_copy(0).start()
    part_copy(0).wait_recv()
    assemble(0)
    assemble(1)

    square = jnp.zeros((block, LANES), f32)
    for j in range(width // LANES):
        v = resid_ref[:, pl.ds(j * LANES, LANES)]
        square = square + v * v
    inv = lax.rsqrt(jnp.sum(square, axis=1, keepdims=True) / width + eps_norm)
    for c in range(ring):
        cols = pl.ds(c * chip_cols, chip_cols)
        gain = gain_of(mgain_ref, c)
        x_ref[:, cols] = (resid_ref[:, cols] * inv * gain).astype(bf16)

    hid_copy.wait_send()

    def drain_ring(step, carry):
        for kind in ("kv", "wo"):
            for flow in range(2):
                for piece in range(2):
                    ring_copy(kind, kinds[kind][0].at[0], step, flow, piece).wait_send()
        return carry

    lax.fori_loop(1, half, drain_ring, 0)
    for kind in ("kv", "wo"):
        for flow in range(2):
            ring_copy(kind, kinds[kind][0].at[0], half, flow, flow).wait_send()

    def drain_sides(slot, carry):
        for kind in ("kv", "wo"):
            for axis in range(2):
                side_copy(kind, slot, axis).wait_send()
        return carry

    lax.fori_loop(1, ring, drain_sides, 0)

    def drain_parts(g, carry):
        part_copy(g).wait_send()
        return carry

    lax.fori_loop(0, half, drain_parts, 0)


def prelude(hidden, queries, cache, cache_lengths, wkv, wo, attn_gain, moe_gain, expert_ids, gates):
    ring = lax.axis_size("tok")
    half = ring // 2
    side = math.isqrt(lax.axis_size("grp"))
    span, wide_half = hidden.shape
    block, width = span // 2, 2 * wide_half
    heads, head_dim = queries.shape[1:]
    positions, kv_heads = cache.shape[1:3]
    four = 2 * kv_heads
    chip_cols = width // ring
    rows = heads // kv_heads * span
    vmem = pl.BlockSpec(memory_space=pltpu.VMEM)
    hbm = pl.BlockSpec(memory_space=pltpu.HBM)
    smem = pl.BlockSpec(memory_space=pltpu.SMEM)
    dma = pltpu.SemaphoreType.DMA
    depth = heads * head_dim // 4
    return pl.pallas_call(
        functools.partial(prelude_kernel, half, side),
        out_shape=(
            jax.ShapeDtypeStruct((block, width + LANES), bf16),
            jax.ShapeDtypeStruct((block, width), f32),
            jax.ShapeDtypeStruct((span * four, head_dim), bf16),
        ),
        in_specs=[vmem, vmem, hbm, smem, vmem, vmem, vmem, vmem, vmem, vmem],
        out_specs=(vmem, vmem, vmem),
        scratch_shapes=[
            pltpu.VMEM((span, four * head_dim), bf16),
            pltpu.VMEM((2, span, wide_half), bf16),
            pltpu.VMEM((ring, span, chip_cols), bf16),
            pltpu.VMEM((ring, 4, chip_cols // 4, four * head_dim), bf16),
            pltpu.VMEM((ring, 4, depth, chip_cols), bf16),
            pltpu.VMEM((positions * four, head_dim), bf16),
            pltpu.VMEM((kv_heads, positions, head_dim), bf16),
            pltpu.VMEM((kv_heads, positions, head_dim), bf16),
            pltpu.VMEM((heads, span, head_dim), bf16),
            pltpu.VMEM((span, four * head_dim), f32),
            pltpu.VMEM((kv_heads, rows, LANES), f32),
            pltpu.VMEM((kv_heads, rows, LANES), f32),
            pltpu.VMEM((kv_heads, rows, head_dim), f32),
            pltpu.VMEM((span, heads * head_dim), bf16),
            pltpu.VMEM((2, ring, block, chip_cols), f32),
            pltpu.VMEM((ring, block, chip_cols), f32),
            dma((1,)),
            dma((1,)),
            dma((1,)),
            dma((half + 1, 2, 2)),
            dma((half + 1, 2, 2)),
            dma((ring, 2)),
            dma((ring, 2)),
            dma((half + 1, 2, 2)),
            dma((half + 1, 2, 2)),
            dma((ring, 2)),
            dma((ring, 2)),
            dma((half,)),
            dma((half,)),
        ],
        compiler_params=pltpu.CompilerParams(
            collective_id=0, has_side_effects=True, vmem_limit_bytes=67043328
        ),
        name="prelude",
    )(
        hidden,
        queries.reshape(span // 32, 32 * heads, head_dim),
        cache.reshape(positions * four, head_dim),
        cache_lengths,
        wkv.reshape(4, chip_cols // 4 * four, head_dim),
        wo.reshape(4, depth, chip_cols),
        attn_gain.reshape(width // LANES, LANES),
        moe_gain.reshape(width // LANES, LANES),
        expert_ids.T,
        gates.T,
    )


PIECES = 2


def expert_kernel(
    half,
    x_ref,
    resid_ref,
    wg_hbm,
    wu_hbm,
    wd_hbm,
    out_ref,
    xs,
    wgu,
    wd,
    gu,
    hid,
    mine,
    pout,
    pin,
    rsin,
    wsem,
    ag_send,
    ag_recv,
    x_send,
    x_recv,
    p_send,
    p_recv,
    rs_send,
    rs_recv,
):
    ring = 2 * half
    z = lax.axis_index("tok")
    m = lax.axis_index("mdl")
    ahead = lax.rem(z + 1, ring)
    behind = lax.rem(z + ring - 1, ring)
    partner = {"mdl": 1 - m}
    expert = z // (ring // EXPERTS)
    block, width = resid_ref.shape
    ffs = wg_hbm.shape[1]
    cut = width // PIECES
    spans = [(i * cut, cut) for i in range(PIECES)]
    wide_spans = spans[:-1] + [(width - cut, cut + LANES)]
    side_of = [i * 2 // PIECES for i in range(PIECES)]

    loads = (
        pltpu.make_async_copy(wg_hbm, wgu.at[:, pl.ds(0, ffs)], wsem.at[0]),
        pltpu.make_async_copy(wu_hbm, wgu.at[:, pl.ds(ffs, ffs)], wsem.at[1]),
        pltpu.make_async_copy(wd_hbm, wd, wsem.at[2]),
    )

    barrier = pltpu.get_barrier_semaphore()
    for who in ({"tok": ahead}, {"tok": behind}, partner):
        pl.semaphore_signal(barrier, inc=1, device_id=who, device_id_type=MESH)
    pl.semaphore_wait(barrier, 3)

    def ring_copy(src, dst_slot, flow, piece, step):
        cols = pl.ds(*wide_spans[piece])
        return pltpu.make_async_remote_copy(
            src_ref=src.at[:, cols],
            dst_ref=xs.at[dst_slot, 0, :, cols],
            send_sem=ag_send.at[step, flow, piece],
            recv_sem=ag_recv.at[step, flow, piece],
            device_id={"tok": behind if flow == 0 else ahead},
            device_id_type=MESH,
        )

    def partner_copy(src, slot, piece):
        cols = pl.ds(*wide_spans[piece])
        return pltpu.make_async_remote_copy(
            src_ref=src.at[:, cols],
            dst_ref=xs.at[slot, 1, :, cols],
            send_sem=x_send.at[slot, piece],
            recv_sem=x_recv.at[slot, piece],
            device_id=partner,
            device_id_type=MESH,
        )

    for piece in range(PIECES):
        for flow in range(2):
            ring_copy(x_ref, 2 + flow, flow, piece, 1).start()
    for load in loads:
        load.start()
    for piece in range(PIECES):
        partner_copy(x_ref, 0, piece).start()
    xs[0, 0] = x_ref[...]

    def gate_up(g):
        rows = xs[pl.ds(2 * g, 2), :, :, pl.ds(0, width)].reshape(4 * block, width)
        gu[...] = jnp.dot(rows, wgu[...], preferred_element_type=f32)

    def activate():
        gate = gu[:, pl.ds(0, ffs)]
        up = gu[:, pl.ds(ffs, ffs)]
        hid[...] = (gate / (1.0 + jnp.exp(-gate)) * up).astype(bf16)

    def weight_of(g):
        tail = xs[pl.ds(2 * g, 2), :, :, pl.ds(width, LANES)].reshape(4 * block, LANES)
        lane = lax.broadcasted_iota(jnp.int32, (4 * block, LANES), 1)
        pick = (lane == expert) | (lane == expert + EXPERTS)
        return jnp.sum(jnp.where(pick, tail.astype(f32), 0.0), axis=1, keepdims=True)

    def down(g, side):
        weight = weight_of(g)
        cols = pl.ds(side * (width // 2), width // 2)
        got = jnp.dot(hid[...], wd[:, cols], preferred_element_type=f32) * weight
        got = got.astype(bf16)
        for slot in range(2):
            mine[2 * g + slot, :, cols] = got[2 * slot * block : (2 * slot + 1) * block]
            pout[2 * g + slot, :, cols] = got[(2 * slot + 1) * block : (2 * slot + 2) * block]

    def give(g, side):
        cols = pl.ds(side * (width // 2), width // 2)
        return pltpu.make_async_remote_copy(
            src_ref=pout.at[pl.ds(2 * g, 2), :, cols],
            dst_ref=pin.at[pl.ds(2 * g, 2), :, cols],
            send_sem=p_send.at[g, side],
            recv_sem=p_recv.at[g, side],
            device_id=partner,
            device_id_type=MESH,
        )

    def await_partner(g):
        for slot in range(2):
            for piece in range(PIECES):
                partner_copy(x_ref, 2 * g + slot, piece).wait_recv()

    def arrive(s, flow, piece, onward):
        ring_copy(x_ref, 2 * s + flow, flow, piece, s).wait_recv()
        if onward is not None:
            ring_copy(xs.at[2 * s + flow, 0], onward, flow, piece, s + 1).start()
        partner_copy(xs.at[2 * s + flow, 0], 2 * s + flow, piece).start()

    for piece in range(PIECES):
        for flow in range(2):
            arrive(1, flow, piece, 4 + flow)
        if piece == 0:
            for load in loads:
                load.wait()

    last = half - 1

    def events(s, piece):
        @pl.when(s < last)
        def _():
            for flow in range(2):
                arrive(s, flow, piece, 2 * (s + 1) + flow)

        @pl.when(s == last)
        def _():
            for flow in range(2):
                arrive(last, flow, piece, 1 if flow == side_of[piece] else None)

        @pl.when(s == half)
        def _():
            ring_copy(x_ref, 1, side_of[piece], piece, half).wait_recv()
            partner_copy(xs.at[1, 0], 1, piece).start()

    def body(s, carry):
        g = lax.rem(s - 1, half)
        for piece in range(PIECES // 2):
            events(s, piece)
        await_partner(g)
        gate_up(g)
        for piece in range(PIECES // 2, PIECES):
            events(s, piece)
        activate()
        for side in range(2):
            down(g, side)
            give(g, side).start()
        return carry

    lax.fori_loop(2, half + 2, body, 0)

    def sum_copy(slot, flow, piece, step):
        cols = pl.ds(*spans[piece])
        return pltpu.make_async_remote_copy(
            src_ref=mine.at[slot, :, cols],
            dst_ref=rsin.at[flow, step, :, cols],
            send_sem=rs_send.at[step, flow, piece],
            recv_sem=rs_recv.at[step, flow, piece],
            device_id={"tok": ahead if flow == 0 else behind},
            device_id_type=MESH,
        )

    def add_and_send(slot, flow, piece, step, incoming):
        cols = pl.ds(*spans[piece])
        total = mine[slot, :, cols].astype(f32) + pin[slot, :, cols].astype(f32)
        if incoming:
            sum_copy(slot, flow, piece, step - 1).wait_recv()
            total = total + rsin[flow, step - 1, :, cols].astype(f32)
        mine[slot, :, cols] = total.astype(bf16)
        sum_copy(slot, flow, piece, step).start()

    for flow in range(2):
        give(0, flow).wait_recv()
        for piece in range(PIECES):
            if side_of[piece] == flow:
                add_and_send(1, flow, piece, 0, False)
    for flow in range(2):
        give(last, flow).wait_recv()
    for incoming in (False, True):
        for piece in range(PIECES):
            flow = side_of[piece] if incoming else 1 - side_of[piece]
            add_and_send(2 * last + flow, flow, piece, 1, incoming)

    def fold(step, carry):
        s = half - step
        for side in range(2):
            give(s, side).wait_recv()
        for piece in range(PIECES):
            for flow in range(2):
                add_and_send(2 * s + flow, flow, piece, step, True)
        return carry

    lax.fori_loop(2, half, fold, 0)

    for piece in range(PIECES):
        cols = pl.ds(*spans[piece])
        total = resid_ref[:, cols] + mine[0, :, cols].astype(f32) + pin[0, :, cols].astype(f32)
        for flow in range(2):
            sum_copy(0, flow, piece, half - 1).wait_recv()
            total = total + rsin[flow, half - 1, :, cols].astype(f32)
        out_ref[:, cols] = total.astype(bf16)

    def drain_ring(s, carry):
        for flow in range(2):
            for piece in range(PIECES):
                ring_copy(x_ref, 1, flow, piece, s).wait_send()
        return carry

    lax.fori_loop(1, half, drain_ring, 0)
    for piece in range(PIECES):
        ring_copy(x_ref, 1, side_of[piece], piece, half).wait_send()

    def drain_slots(slot, carry):
        for piece in range(PIECES):
            partner_copy(x_ref, slot, piece).wait_send()
        return carry

    lax.fori_loop(0, ring, drain_slots, 0)

    def drain_groups(g, carry):
        for side in range(2):
            give(g, side).wait_send()
        return carry

    lax.fori_loop(0, half, drain_groups, 0)

    def drain_sums(step, carry):
        for flow in range(2):
            for piece in range(PIECES):
                sum_copy(0, flow, piece, step).wait_send()
        return carry

    for piece in range(PIECES):
        sum_copy(0, side_of[piece], piece, 0).wait_send()
    lax.fori_loop(1, half, drain_sums, 0)


def expert_layer(x_wide, resid, w_gate, w_up, w_down):
    ring = lax.axis_size("tok")
    half = ring // 2
    block, width = resid.shape
    ffs = w_gate.shape[1]
    wide = x_wide.shape[1]
    vmem = pl.BlockSpec(memory_space=pltpu.VMEM)
    hbm = pl.BlockSpec(memory_space=pltpu.HBM)
    dma = pltpu.SemaphoreType.DMA
    return pl.pallas_call(
        functools.partial(expert_kernel, half),
        out_shape=jax.ShapeDtypeStruct((block, width), bf16),
        in_specs=[vmem, vmem, hbm, hbm, hbm],
        out_specs=vmem,
        scratch_shapes=[
            pltpu.VMEM((ring, 2, block, wide), bf16),
            pltpu.VMEM((width, 2 * ffs), bf16),
            pltpu.VMEM((ffs, width), bf16),
            pltpu.VMEM((4 * block, 2 * ffs), f32),
            pltpu.VMEM((4 * block, ffs), bf16),
            pltpu.VMEM((ring, block, width), bf16),
            pltpu.VMEM((ring, block, width), bf16),
            pltpu.VMEM((ring, block, width), bf16),
            pltpu.VMEM((2, half, block, width), bf16),
            dma((3,)),
            dma((half + 1, 2, PIECES)),
            dma((half + 1, 2, PIECES)),
            dma((ring, PIECES)),
            dma((ring, PIECES)),
            dma((half, 2)),
            dma((half, 2)),
            dma((half, 2, PIECES)),
            dma((half, 2, PIECES)),
        ],
        compiler_params=pltpu.CompilerParams(
            collective_id=1, has_side_effects=True, vmem_limit_bytes=67043328
        ),
        name="expert_layer",
    )(x_wide, resid, w_gate, w_up, w_down)


def results_kernel(mixed_ref, fresh_ref, mixed_out, fresh_out):
    mixed_out[...] = mixed_ref[...]
    fresh_out[...] = fresh_ref[...]


def results(mixed, fresh):
    vmem = pl.BlockSpec(memory_space=pltpu.VMEM)
    return pl.pallas_call(
        results_kernel,
        out_shape=tuple(jax.ShapeDtypeStruct(v.shape, v.dtype) for v in (mixed, fresh)),
        in_specs=[vmem, vmem],
        out_specs=(vmem, vmem),
        name="results",
    )(mixed, fresh)


def shards(
    hidden,
    queries,
    cache,
    cache_lengths,
    wkv,
    wo,
    attn_gain,
    moe_gain,
    w_gate,
    w_up,
    w_down,
    expert_ids,
    gates,
):
    x_wide, resid, fresh = prelude(
        hidden, queries, cache, cache_lengths, wkv, wo, attn_gain, moe_gain, expert_ids, gates
    )
    mixed = expert_layer(x_wide, resid, w_gate[0], w_up[0], w_down[0])
    mixed, fresh = results(mixed, fresh)
    fresh_key_value = fresh.reshape(hidden.shape[0], *wkv.shape[1:])
    return (mixed, fresh_key_value)


def solution(mesh):
    in_specs = (
        P(("grp", "tok"), "mdl"),
        P(("grp", "tok"), "mdl", None),
        P(("grp", "tok"), None, "mdl", None, None),
        P(("grp", "tok")),
        P("tok", "mdl", None, None),
        P("mdl", None, "tok"),
        P(),
        P(),
        P(("tok", "mdl"), None, None),
        P(("tok", "mdl"), None, None),
        P(("tok", "mdl"), None, None),
        P(("grp", "tok", "mdl"), None),
        P(("grp", "tok", "mdl"), None),
    )
    out_specs = (P(("grp", "tok", "mdl"), None), P(("grp", "tok"), "mdl", None, None))
    return jax.shard_map(shards, mesh=mesh, in_specs=in_specs, out_specs=out_specs, check_vma=False)
```

```python
import functools
import math

import jax
import jax.numpy as jnp
from jax import lax
from jax.experimental import pallas as pl
from jax.experimental.pallas import tpu as pltpu
from jax.sharding import PartitionSpec as P

EXPERTS = 4
TOPK = 2

eps_norm = 1e-05
rope_base = 1000000.0
mask_fill = -1e30

MESH = pl.DeviceIdType.MESH
bf16 = jnp.bfloat16
f32 = jnp.float32


LANES = 128
KEYS = 512


def permutation(groups, size):
    each = size // groups
    row = lax.broadcasted_iota(jnp.int32, (size, size), 0)
    col = lax.broadcasted_iota(jnp.int32, (size, size), 1)
    return jnp.where(col == lax.rem(row, each) * groups + row // each, 1.0, 0.0).astype(bf16)


def prelude_kernel(
    half,
    side,
    hid_ref,
    q_ref,
    cache_hbm,
    len_ref,
    wkv_ref,
    wo_ref,
    again_ref,
    mgain_ref,
    ids_ref,
    gates_ref,
    x_ref,
    resid_ref,
    rows_ref,
    fresh_ref,
    hfull,
    normed,
    kvbuf,
    wobuf,
    raw,
    keys,
    vals,
    qs,
    kvacc,
    smax,
    ssum,
    sacc,
    heads,
    part,
    part_in,
    csem,
    h_send,
    h_recv,
    kv_send,
    kv_recv,
    kvn_send,
    kvn_recv,
    wo_send,
    wo_recv,
    won_send,
    won_recv,
    p_send,
    p_recv,
    end_send,
    end_recv,
    endn_send,
    endn_recv,
):
    ring = 2 * half
    z = lax.axis_index("tok")
    m = lax.axis_index("mdl")
    gid = lax.axis_index("grp")
    ahead = lax.rem(z + 1, ring)
    behind = lax.rem(z + ring - 1, ring)
    odd_a = lax.rem(gid // side, 2)
    odd_b = lax.rem(gid, 2)
    neighbours = ({"grp": gid + side * (1 - 2 * odd_a)}, {"grp": gid + 1 - 2 * odd_b})
    own = 2 * odd_a + odd_b
    quarters = (own, 3 - own)
    partner = {"mdl": 1 - m}
    span, wide_half = hid_ref.shape
    block = span // 2
    width = resid_ref.shape[1]
    chip_cols = width // ring
    kv_heads = keys.shape[0]
    positions = keys.shape[1]
    head_total, _, head_dim = qs.shape
    per_group = head_total // kv_heads
    rows = per_group * span
    scale = 1.0 / math.sqrt(head_dim)

    load = pltpu.make_async_copy(cache_hbm, raw, csem.at[0])
    load.start()

    barrier = pltpu.get_barrier_semaphore()
    for who in ({"tok": ahead}, {"tok": behind}, *neighbours, partner):
        pl.semaphore_signal(barrier, inc=1, device_id=who, device_id_type=MESH)

    four = 2 * kv_heads
    perm4 = permutation(four, 64 * four)
    for q in range(4):
        got = jnp.dot(perm4, wkv_ref[q], preferred_element_type=f32).astype(bf16)
        for j in range(four):
            kvbuf[0, q, :, pl.ds(j * head_dim, head_dim)] = got[j * 64 : (j + 1) * 64]
    pl.semaphore_wait(barrier, 5)

    hid_copy = pltpu.make_async_remote_copy(
        src_ref=hid_ref,
        dst_ref=hfull.at[m],
        send_sem=h_send.at[0],
        recv_sem=h_recv.at[0],
        device_id=partner,
        device_id_type=MESH,
    )
    hid_copy.start()

    kinds = {
        "kv": (kvbuf, kv_send, kv_recv, kvn_send, kvn_recv),
        "wo": (wobuf, wo_send, wo_recv, won_send, won_recv),
    }

    def slot_of(step, flow):
        return 1 if isinstance(step, int) and step == half else 2 * step + flow

    def ring_copy(kind, src, step, flow, piece):
        buf, send, recv, _, _ = kinds[kind]
        q = quarters[piece]
        return pltpu.make_async_remote_copy(
            src_ref=src.at[q],
            dst_ref=buf.at[slot_of(step, flow), q],
            send_sem=send.at[step, flow, piece],
            recv_sem=recv.at[step, flow, piece],
            device_id={"tok": behind if flow == 0 else ahead},
            device_id_type=MESH,
        )

    def side_copy(kind, slot, axis):
        buf, _, _, send, recv = kinds[kind]
        return pltpu.make_async_remote_copy(
            src_ref=buf.at[slot, own],
            dst_ref=buf.at[slot, own],
            send_sem=send.at[slot, axis],
            recv_sem=recv.at[slot, axis],
            device_id=neighbours[axis],
            device_id_type=MESH,
        )

    part_rows = wo_ref.shape[1] // 2

    def end_copy(flow, sub):
        q = quarters[flow]
        at = pl.ds(sub * part_rows, part_rows)
        return pltpu.make_async_remote_copy(
            src_ref=wobuf.at[2 * (half - 1) + flow, q, at],
            dst_ref=wobuf.at[1, q, at],
            send_sem=end_send.at[flow, sub],
            recv_sem=end_recv.at[flow, sub],
            device_id={"tok": behind if flow == 0 else ahead},
            device_id_type=MESH,
        )

    def end_side(axis, sub):
        at = pl.ds(sub * part_rows, part_rows)
        return pltpu.make_async_remote_copy(
            src_ref=wobuf.at[1, own, at],
            dst_ref=wobuf.at[1, own, at],
            send_sem=endn_send.at[axis, sub],
            recv_sem=endn_recv.at[axis, sub],
            device_id=neighbours[axis],
            device_id_type=MESH,
        )

    def arrive(kind, step, pieces=(0, 1)):
        buf = kinds[kind][0]
        for piece in pieces:
            for flow in range(2):
                final = isinstance(step, int) and step == half
                if final and flow != piece:
                    continue
                slot = slot_of(step, flow)
                ring_copy(kind, buf.at[slot], step, flow, piece).wait_recv()
                if not final:
                    turn = isinstance(step, int) and step == half - 1
                    if turn and flow == piece and kind == "wo":
                        for sub in range(2):
                            end_copy(flow, sub).start()
                    elif not turn or flow == piece:
                        ring_copy(kind, buf.at[slot], step + 1, flow, piece).start()
                if piece == 0:
                    for axis in range(2):
                        side_copy(kind, slot, axis).start()

    def settle(kind, slot):
        for axis in range(2):
            side_copy(kind, slot, axis).wait_recv()

    for piece in range(2):
        for flow in range(2):
            ring_copy("kv", kvbuf.at[0], 1, flow, piece).start()
    for piece in range(2):
        for flow in range(2):
            ring_copy("wo", wo_ref, 1, flow, piece).start()

    lane = lax.broadcasted_iota(jnp.int32, (16, block), 0)
    route = jnp.zeros((16, block), f32)
    for k in range(TOPK):
        hit = (ids_ref[k : k + 1, :] == lane) | (ids_ref[k : k + 1, :] + EXPERTS == lane)
        route = route + jnp.where(hit, gates_ref[k : k + 1, :], 0.0)
    high = route.astype(bf16).astype(f32)
    terms = jnp.where(lane < EXPERTS, high, route - high)
    place = lax.broadcasted_iota(jnp.int32, (16, LANES), 0) == lax.broadcasted_iota(
        jnp.int32, (16, LANES), 1
    )
    tail = lax.dot_general(
        terms.astype(bf16),
        jnp.where(place, 1.0, 0.0).astype(bf16),
        (((0,), (0,)), ((), ())),
        preferred_element_type=f32,
    )
    x_ref[:, pl.ds(width, LANES)] = tail.astype(bf16)

    perm_q = permutation(head_total, 32 * head_total)
    for b in range(span // 32):
        got = jnp.dot(perm_q, q_ref[b], preferred_element_type=f32).astype(bf16)
        for h in range(head_total):
            qs[h, pl.ds(32 * b, 32), :] = got[32 * h : 32 * (h + 1)]

    def gain_of(ref, c):
        each = chip_cols // LANES
        gains = [ref[c * each + j : c * each + j + 1, :].astype(f32) for j in range(each)]
        return jnp.concatenate(gains, axis=1)

    hfull[m] = hid_ref[...]
    hid_copy.wait_recv()
    square = jnp.zeros((span, LANES), f32)
    for j in range(width // LANES):
        v = hfull[j // (ring // 2 * chip_cols // LANES), :, pl.ds(j * LANES % wide_half, LANES)]
        v = v.astype(f32)
        square = square + v * v
    inv = lax.rsqrt(jnp.sum(square, axis=1, keepdims=True) / width + eps_norm)
    for c in range(ring):
        v = hfull[c * chip_cols // wide_half, :, pl.ds(c * chip_cols % wide_half, chip_cols)]
        gain = gain_of(again_ref, c)
        normed[c] = (v.astype(f32) * inv * gain).astype(bf16)

    def chip_of(slot):
        if isinstance(slot, int) and slot < 2:
            return lax.rem(z + slot * half, ring)
        step, flow = slot // 2, lax.rem(slot, 2)
        return lax.rem(z + ring + step * (1 - 2 * flow), ring)

    def kv_use(slot):
        weights = kvbuf[slot].reshape(chip_cols, four * head_dim)
        kvacc[...] += jnp.dot(normed[chip_of(slot)], weights, preferred_element_type=f32)

    kvacc[...] = jnp.zeros_like(kvacc)
    kv_use(0)

    load.wait()

    def unpack(b, carry):
        got = jnp.dot(
            perm4,
            raw[pl.ds(pl.multiple_of(b * 64 * four, 64 * four), 64 * four), :],
            preferred_element_type=f32,
        ).astype(bf16)
        at = pl.ds(pl.multiple_of(b * 64, 64), 64)
        for g in range(kv_heads):
            keys[g, at, :] = got[(2 * g) * 64 : (2 * g + 1) * 64]
            vals[g, at, :] = got[(2 * g + 1) * 64 : (2 * g + 2) * 64]
        return carry

    lax.fori_loop(0, positions // 64, unpack, 0)

    length = len_ref[0]
    smax[...] = jnp.full_like(smax, mask_fill)
    ssum[...] = jnp.zeros_like(ssum)
    sacc[...] = jnp.zeros_like(sacc)

    def attend(g, key_rows, value_rows, allowed):
        query_rows = qs[pl.ds(per_group * g, per_group)].reshape(rows, head_dim)
        scores = lax.dot_general(
            query_rows, key_rows, (((1,), (1,)), ((), ())), preferred_element_type=f32
        )
        scores = jnp.where(allowed, scores * scale, mask_fill)
        old = smax[g][:, :1]
        top = jnp.maximum(old, jnp.max(scores, axis=1, keepdims=True))
        weights = jnp.where(allowed, jnp.exp(scores - top), 0.0)
        fade = jnp.exp(old - top)
        smax[g] = jnp.broadcast_to(top, (rows, LANES))
        ssum[g] = ssum[g] * fade + jnp.sum(weights, axis=1, keepdims=True)
        sacc[g] = sacc[g] * fade + jnp.dot(
            weights.astype(bf16), value_rows, preferred_element_type=f32
        )

    key_blocks = positions // KEYS

    def cached(i):
        g = i // key_blocks
        lo = lax.rem(i, key_blocks) * KEYS
        if not isinstance(lo, int):
            lo = pl.multiple_of(lo, KEYS)
        col = lo + lax.broadcasted_iota(jnp.int32, (rows, KEYS), 1)
        attend(g, keys[g, pl.ds(lo, KEYS), :], vals[g, pl.ds(lo, KEYS), :], col < length)

    def kv_step(step):
        arrive("kv", step)
        cached(step - 1)

    def kv_settled(step):
        for flow in range(2):
            settle("kv", slot_of(step, flow))
            kv_use(slot_of(step, flow))

    kv_step(1)
    arrive("wo", 1, (0,))

    def pair(k):
        kv_step(2 * k)
        arrive("wo", k, (1,))
        kv_settled(2 * k - 1)
        kv_step(2 * k + 1)
        arrive("wo", k + 1, (0,))
        kv_settled(2 * k)

    def pairs(k, carry):
        pair(k)
        return carry

    lax.fori_loop(1, half // 2 - 1, pairs, 0)
    pair(half // 2 - 1)
    arrive("kv", half)
    arrive("wo", half // 2, (1,))
    kv_settled(half - 1)
    cached(jnp.int32(half - 1))
    settle("kv", 1)
    kv_use(1)

    lanes = lax.broadcasted_iota(jnp.int32, (span, head_dim), 1)
    place_of = lax.broadcasted_iota(jnp.int32, (span, head_dim), 0) + length
    pair_of = lax.rem(lanes, head_dim // 2).astype(f32)
    angle = place_of.astype(f32) * jnp.exp(pair_of * (-2.0 * math.log(rope_base) / head_dim))
    cosine = jnp.cos(angle)
    sine = jnp.where(lanes < head_dim // 2, -jnp.sin(angle), jnp.sin(angle))
    token = lax.rem(lax.broadcasted_iota(jnp.int32, (rows, span), 0), span)
    causal = lax.broadcasted_iota(jnp.int32, (rows, span), 1) <= token
    for g in range(kv_heads):
        k_cols = pl.ds(2 * g * head_dim, head_dim)
        v_cols = pl.ds((2 * g + 1) * head_dim, head_dim)
        key = kvacc[:, k_cols]
        turned = pltpu.roll(key, head_dim // 2, 1)
        fresh_ref[:, k_cols] = (key * cosine + turned * sine).astype(bf16)
        fresh_ref[:, v_cols] = kvacc[:, v_cols].astype(bf16)
        attend(g, fresh_ref[:, k_cols], fresh_ref[:, v_cols], causal)
        done = (sacc[g] / ssum[g]).astype(bf16)
        for h in range(per_group):
            at = pl.ds((g * per_group + h) * head_dim, head_dim)
            heads[:, at] = done[h * span : (h + 1) * span]

    columns = [fresh_ref[:, pl.ds(j * head_dim, head_dim)] for j in range(four)]
    rows_ref[...] = lax.dot_general(
        perm4,
        jnp.concatenate(columns, axis=0),
        (((0,), (0,)), ((), ())),
        preferred_element_type=f32,
    ).astype(bf16)

    def wo_use(slot, buf):
        weights = buf.reshape(4 * wo_ref.shape[1], chip_cols)
        got = jnp.dot(heads[...], weights, preferred_element_type=f32)
        for core in range(2):
            part[core, slot] = got[core * block : (core + 1) * block]

    def part_copy(g):
        return pltpu.make_async_remote_copy(
            src_ref=part.at[1 - m, pl.ds(2 * g, 2)],
            dst_ref=part_in.at[pl.ds(2 * g, 2)],
            send_sem=p_send.at[g],
            recv_sem=p_recv.at[g],
            device_id=partner,
            device_id_type=MESH,
        )

    def wo_settled(step):
        for flow in range(2):
            slot = slot_of(step, flow)
            settle("wo", slot)
            wo_use(slot, wobuf[slot])
        part_copy(step).start()

    def assemble(slot):
        c = chip_of(slot)
        cols = pl.ds(pl.multiple_of(c * chip_cols, chip_cols), chip_cols)
        in_half = pl.ds(
            pl.multiple_of(lax.rem(c * chip_cols, wide_half), chip_cols), chip_cols
        )
        mine = hfull[c * chip_cols // wide_half, pl.ds(pl.multiple_of(m * block, block), block), in_half]
        resid_ref[:, cols] = mine.astype(f32) + part[m, slot] + part_in[slot]

    def gather_parts(step):
        part_copy(step).wait_recv()
        for flow in range(2):
            assemble(slot_of(step, flow))

    wo_use(0, wo_ref[...])

    def late(s, carry):
        arrive("wo", s)
        first = 2 * (s - half // 2) - 1
        wo_settled(first)
        wo_settled(first + 1)
        return carry

    lax.fori_loop(half // 2 + 1, half - 1, late, 0)
    arrive("wo", half - 1)
    wo_settled(half - 3)

    def early(step, carry):
        gather_parts(step)
        return carry

    lax.fori_loop(1, half - 3, early, 0)
    for sub in range(2):
        end_copy(0, sub).wait_recv()
        for axis in range(2):
            end_side(axis, sub).start()
    for sub in range(2):
        end_copy(1, sub).wait_recv()
    wo_settled(half - 2)
    wo_settled(half - 1)
    lax.fori_loop(half - 3, half, early, 0)
    for sub in range(2):
        for axis in range(2):
            end_side(axis, sub).wait_recv()
    wo_use(1, wobuf[1])
    part_copy(0).start()
    part_copy(0).wait_recv()
    assemble(0)
    assemble(1)

    square = jnp.zeros((block, LANES), f32)
    for j in range(width // LANES):
        v = resid_ref[:, pl.ds(j * LANES, LANES)]
        square = square + v * v
    inv = lax.rsqrt(jnp.sum(square, axis=1, keepdims=True) / width + eps_norm)
    for c in range(ring):
        cols = pl.ds(c * chip_cols, chip_cols)
        gain = gain_of(mgain_ref, c)
        x_ref[:, cols] = (resid_ref[:, cols] * inv * gain).astype(bf16)

    hid_copy.wait_send()

    def drain_ring(step, carry):
        for kind in ("kv", "wo"):
            for flow in range(2):
                for piece in range(2):
                    ring_copy(kind, kinds[kind][0].at[0], step, flow, piece).wait_send()
        return carry

    lax.fori_loop(1, half, drain_ring, 0)
    for flow in range(2):
        ring_copy("kv", kvbuf.at[0], half, flow, flow).wait_send()
        for sub in range(2):
            end_copy(flow, sub).wait_send()
            end_side(flow, sub).wait_send()

    def drain_sides(slot, carry):
        for kind in ("kv", "wo"):
            for axis in range(2):
                side_copy(kind, slot, axis).wait_send()
        return carry

    for axis in range(2):
        side_copy("kv", 1, axis).wait_send()
    lax.fori_loop(2, ring, drain_sides, 0)

    def drain_parts(g, carry):
        part_copy(g).wait_send()
        return carry

    lax.fori_loop(0, half, drain_parts, 0)


def prelude(hidden, queries, cache, cache_lengths, wkv, wo, attn_gain, moe_gain, expert_ids, gates):
    ring = lax.axis_size("tok")
    half = ring // 2
    side = math.isqrt(lax.axis_size("grp"))
    span, wide_half = hidden.shape
    block, width = span // 2, 2 * wide_half
    heads, head_dim = queries.shape[1:]
    positions, kv_heads = cache.shape[1:3]
    four = 2 * kv_heads
    chip_cols = width // ring
    rows = heads // kv_heads * span
    vmem = pl.BlockSpec(memory_space=pltpu.VMEM)
    hbm = pl.BlockSpec(memory_space=pltpu.HBM)
    smem = pl.BlockSpec(memory_space=pltpu.SMEM)
    dma = pltpu.SemaphoreType.DMA
    depth = heads * head_dim // 4
    return pl.pallas_call(
        functools.partial(prelude_kernel, half, side),
        out_shape=(
            jax.ShapeDtypeStruct((block, width + LANES), bf16),
            jax.ShapeDtypeStruct((block, width), f32),
            jax.ShapeDtypeStruct((span * four, head_dim), bf16),
        ),
        in_specs=[vmem, vmem, hbm, smem, vmem, vmem, vmem, vmem, vmem, vmem],
        out_specs=(vmem, vmem, vmem),
        scratch_shapes=[
            pltpu.VMEM((span, four * head_dim), bf16),
            pltpu.VMEM((2, span, wide_half), bf16),
            pltpu.VMEM((ring, span, chip_cols), bf16),
            pltpu.VMEM((ring, 4, chip_cols // 4, four * head_dim), bf16),
            pltpu.VMEM((ring, 4, depth, chip_cols), bf16),
            pltpu.VMEM((positions * four, head_dim), bf16),
            pltpu.VMEM((kv_heads, positions, head_dim), bf16),
            pltpu.VMEM((kv_heads, positions, head_dim), bf16),
            pltpu.VMEM((heads, span, head_dim), bf16),
            pltpu.VMEM((span, four * head_dim), f32),
            pltpu.VMEM((kv_heads, rows, LANES), f32),
            pltpu.VMEM((kv_heads, rows, LANES), f32),
            pltpu.VMEM((kv_heads, rows, head_dim), f32),
            pltpu.VMEM((span, heads * head_dim), bf16),
            pltpu.VMEM((2, ring, block, chip_cols), f32),
            pltpu.VMEM((ring, block, chip_cols), f32),
            dma((1,)),
            dma((1,)),
            dma((1,)),
            dma((half + 1, 2, 2)),
            dma((half + 1, 2, 2)),
            dma((ring, 2)),
            dma((ring, 2)),
            dma((half + 1, 2, 2)),
            dma((half + 1, 2, 2)),
            dma((ring, 2)),
            dma((ring, 2)),
            dma((half,)),
            dma((half,)),
            dma((2, 2)),
            dma((2, 2)),
            dma((2, 2)),
            dma((2, 2)),
        ],
        compiler_params=pltpu.CompilerParams(
            collective_id=0, has_side_effects=True, vmem_limit_bytes=67043328
        ),
        name="prelude",
    )(
        hidden,
        queries.reshape(span // 32, 32 * heads, head_dim),
        cache.reshape(positions * four, head_dim),
        cache_lengths,
        wkv.reshape(4, chip_cols // 4 * four, head_dim),
        wo.reshape(4, depth, chip_cols),
        attn_gain.reshape(width // LANES, LANES),
        moe_gain.reshape(width // LANES, LANES),
        expert_ids.T,
        gates.T,
    )


PIECES = 2


def expert_kernel(
    half,
    x_ref,
    resid_ref,
    wg_hbm,
    wu_hbm,
    wd_hbm,
    out_ref,
    xs,
    wgu,
    wd,
    gu,
    hid,
    mine,
    pout,
    pin,
    rsin,
    wsem,
    ag_send,
    ag_recv,
    x_send,
    x_recv,
    p_send,
    p_recv,
    rs_send,
    rs_recv,
):
    ring = 2 * half
    z = lax.axis_index("tok")
    m = lax.axis_index("mdl")
    ahead = lax.rem(z + 1, ring)
    behind = lax.rem(z + ring - 1, ring)
    partner = {"mdl": 1 - m}
    expert = z // (ring // EXPERTS)
    block, width = resid_ref.shape
    ffs = wg_hbm.shape[1]
    cut = width // PIECES
    spans = [(i * cut, cut) for i in range(PIECES)]
    wide_spans = spans[:-1] + [(width - cut, cut + LANES)]
    side_of = [i * 2 // PIECES for i in range(PIECES)]

    loads = (
        pltpu.make_async_copy(wg_hbm, wgu.at[:, pl.ds(0, ffs)], wsem.at[0]),
        pltpu.make_async_copy(wu_hbm, wgu.at[:, pl.ds(ffs, ffs)], wsem.at[1]),
        pltpu.make_async_copy(wd_hbm, wd, wsem.at[2]),
    )

    barrier = pltpu.get_barrier_semaphore()
    for who in ({"tok": ahead}, {"tok": behind}, partner):
        pl.semaphore_signal(barrier, inc=1, device_id=who, device_id_type=MESH)
    pl.semaphore_wait(barrier, 3)

    def ring_copy(src, dst_slot, flow, piece, step):
        cols = pl.ds(*wide_spans[piece])
        return pltpu.make_async_remote_copy(
            src_ref=src.at[:, cols],
            dst_ref=xs.at[dst_slot, 0, :, cols],
            send_sem=ag_send.at[step, flow, piece],
            recv_sem=ag_recv.at[step, flow, piece],
            device_id={"tok": behind if flow == 0 else ahead},
            device_id_type=MESH,
        )

    def partner_copy(src, slot, piece):
        cols = pl.ds(*wide_spans[piece])
        return pltpu.make_async_remote_copy(
            src_ref=src.at[:, cols],
            dst_ref=xs.at[slot, 1, :, cols],
            send_sem=x_send.at[slot, piece],
            recv_sem=x_recv.at[slot, piece],
            device_id=partner,
            device_id_type=MESH,
        )

    for piece in range(PIECES):
        for flow in range(2):
            ring_copy(x_ref, 2 + flow, flow, piece, 1).start()
    for load in loads:
        load.start()
    for piece in range(PIECES):
        partner_copy(x_ref, 0, piece).start()
    xs[0, 0] = x_ref[...]

    def gate_up(g):
        rows = xs[pl.ds(2 * g, 2), :, :, pl.ds(0, width)].reshape(4 * block, width)
        gu[...] = jnp.dot(rows, wgu[...], preferred_element_type=f32)

    def activate():
        gate = gu[:, pl.ds(0, ffs)]
        up = gu[:, pl.ds(ffs, ffs)]
        hid[...] = (gate / (1.0 + jnp.exp(-gate)) * up).astype(bf16)

    def weight_of(g):
        tail = xs[pl.ds(2 * g, 2), :, :, pl.ds(width, LANES)].reshape(4 * block, LANES)
        lane = lax.broadcasted_iota(jnp.int32, (4 * block, LANES), 1)
        pick = (lane == expert) | (lane == expert + EXPERTS)
        return jnp.sum(jnp.where(pick, tail.astype(f32), 0.0), axis=1, keepdims=True)

    def down(g, side):
        weight = weight_of(g)
        cols = pl.ds(side * (width // 2), width // 2)
        got = jnp.dot(hid[...], wd[:, cols], preferred_element_type=f32) * weight
        got = got.astype(bf16)
        for slot in range(2):
            mine[2 * g + slot, :, cols] = got[2 * slot * block : (2 * slot + 1) * block]
            pout[2 * g + slot, :, cols] = got[(2 * slot + 1) * block : (2 * slot + 2) * block]

    def give(g, side):
        cols = pl.ds(side * (width // 2), width // 2)
        return pltpu.make_async_remote_copy(
            src_ref=pout.at[pl.ds(2 * g, 2), :, cols],
            dst_ref=pin.at[pl.ds(2 * g, 2), :, cols],
            send_sem=p_send.at[g, side],
            recv_sem=p_recv.at[g, side],
            device_id=partner,
            device_id_type=MESH,
        )

    def await_partner(g):
        for slot in range(2):
            for piece in range(PIECES):
                partner_copy(x_ref, 2 * g + slot, piece).wait_recv()

    def arrive(s, flow, piece, onward):
        ring_copy(x_ref, 2 * s + flow, flow, piece, s).wait_recv()
        if onward is not None:
            ring_copy(xs.at[2 * s + flow, 0], onward, flow, piece, s + 1).start()
        partner_copy(xs.at[2 * s + flow, 0], 2 * s + flow, piece).start()

    for piece in range(PIECES):
        for flow in range(2):
            arrive(1, flow, piece, 4 + flow)
        if piece == 0:
            for load in loads:
                load.wait()

    last = half - 1

    def events(s, piece):
        @pl.when(s < last)
        def _():
            for flow in range(2):
                arrive(s, flow, piece, 2 * (s + 1) + flow)

        @pl.when(s == last)
        def _():
            for flow in range(2):
                arrive(last, flow, piece, 1 if flow == side_of[piece] else None)

        @pl.when(s == half)
        def _():
            ring_copy(x_ref, 1, side_of[piece], piece, half).wait_recv()
            partner_copy(xs.at[1, 0], 1, piece).start()

    def body(s, carry):
        g = lax.rem(s - 1, half)
        for piece in range(PIECES // 2):
            events(s, piece)
        await_partner(g)
        gate_up(g)
        for piece in range(PIECES // 2, PIECES):
            events(s, piece)
        activate()
        for side in range(2):
            down(g, side)
            give(g, side).start()
        return carry

    lax.fori_loop(2, half + 2, body, 0)

    def sum_copy(slot, flow, piece, step):
        cols = pl.ds(*spans[piece])
        return pltpu.make_async_remote_copy(
            src_ref=mine.at[slot, :, cols],
            dst_ref=rsin.at[flow, step, :, cols],
            send_sem=rs_send.at[step, flow, piece],
            recv_sem=rs_recv.at[step, flow, piece],
            device_id={"tok": ahead if flow == 0 else behind},
            device_id_type=MESH,
        )

    def add_and_send(slot, flow, piece, step, incoming):
        cols = pl.ds(*spans[piece])
        total = mine[slot, :, cols].astype(f32) + pin[slot, :, cols].astype(f32)
        if incoming:
            sum_copy(slot, flow, piece, step - 1).wait_recv()
            total = total + rsin[flow, step - 1, :, cols].astype(f32)
        mine[slot, :, cols] = total.astype(bf16)
        sum_copy(slot, flow, piece, step).start()

    for flow in range(2):
        give(0, flow).wait_recv()
        for piece in range(PIECES):
            if side_of[piece] == flow:
                add_and_send(1, flow, piece, 0, False)
    for flow in range(2):
        give(last, flow).wait_recv()
    for incoming in (False, True):
        for piece in range(PIECES):
            flow = side_of[piece] if incoming else 1 - side_of[piece]
            add_and_send(2 * last + flow, flow, piece, 1, incoming)

    def fold(step, carry):
        s = half - step
        for side in range(2):
            give(s, side).wait_recv()
        for piece in range(PIECES):
            for flow in range(2):
                add_and_send(2 * s + flow, flow, piece, step, True)
        return carry

    lax.fori_loop(2, half, fold, 0)

    for piece in range(PIECES):
        cols = pl.ds(*spans[piece])
        total = resid_ref[:, cols] + mine[0, :, cols].astype(f32) + pin[0, :, cols].astype(f32)
        for flow in range(2):
            sum_copy(0, flow, piece, half - 1).wait_recv()
            total = total + rsin[flow, half - 1, :, cols].astype(f32)
        out_ref[:, cols] = total.astype(bf16)

    def drain_ring(s, carry):
        for flow in range(2):
            for piece in range(PIECES):
                ring_copy(x_ref, 1, flow, piece, s).wait_send()
        return carry

    lax.fori_loop(1, half, drain_ring, 0)
    for piece in range(PIECES):
        ring_copy(x_ref, 1, side_of[piece], piece, half).wait_send()

    def drain_slots(slot, carry):
        for piece in range(PIECES):
            partner_copy(x_ref, slot, piece).wait_send()
        return carry

    lax.fori_loop(0, ring, drain_slots, 0)

    def drain_groups(g, carry):
        for side in range(2):
            give(g, side).wait_send()
        return carry

    lax.fori_loop(0, half, drain_groups, 0)

    def drain_sums(step, carry):
        for flow in range(2):
            for piece in range(PIECES):
                sum_copy(0, flow, piece, step).wait_send()
        return carry

    for piece in range(PIECES):
        sum_copy(0, side_of[piece], piece, 0).wait_send()
    lax.fori_loop(1, half, drain_sums, 0)


def expert_layer(x_wide, resid, w_gate, w_up, w_down):
    ring = lax.axis_size("tok")
    half = ring // 2
    block, width = resid.shape
    ffs = w_gate.shape[1]
    wide = x_wide.shape[1]
    vmem = pl.BlockSpec(memory_space=pltpu.VMEM)
    hbm = pl.BlockSpec(memory_space=pltpu.HBM)
    dma = pltpu.SemaphoreType.DMA
    return pl.pallas_call(
        functools.partial(expert_kernel, half),
        out_shape=jax.ShapeDtypeStruct((block, width), bf16),
        in_specs=[vmem, vmem, hbm, hbm, hbm],
        out_specs=vmem,
        scratch_shapes=[
            pltpu.VMEM((ring, 2, block, wide), bf16),
            pltpu.VMEM((width, 2 * ffs), bf16),
            pltpu.VMEM((ffs, width), bf16),
            pltpu.VMEM((4 * block, 2 * ffs), f32),
            pltpu.VMEM((4 * block, ffs), bf16),
            pltpu.VMEM((ring, block, width), bf16),
            pltpu.VMEM((ring, block, width), bf16),
            pltpu.VMEM((ring, block, width), bf16),
            pltpu.VMEM((2, half, block, width), bf16),
            dma((3,)),
            dma((half + 1, 2, PIECES)),
            dma((half + 1, 2, PIECES)),
            dma((ring, PIECES)),
            dma((ring, PIECES)),
            dma((half, 2)),
            dma((half, 2)),
            dma((half, 2, PIECES)),
            dma((half, 2, PIECES)),
        ],
        compiler_params=pltpu.CompilerParams(
            collective_id=1, has_side_effects=True, vmem_limit_bytes=67043328
        ),
        name="expert_layer",
    )(x_wide, resid, w_gate, w_up, w_down)


def results_kernel(mixed_ref, fresh_ref, mixed_out, fresh_out):
    mixed_out[...] = mixed_ref[...]
    fresh_out[...] = fresh_ref[...]


def results(mixed, fresh):
    vmem = pl.BlockSpec(memory_space=pltpu.VMEM)
    return pl.pallas_call(
        results_kernel,
        out_shape=tuple(jax.ShapeDtypeStruct(v.shape, v.dtype) for v in (mixed, fresh)),
        in_specs=[vmem, vmem],
        out_specs=(vmem, vmem),
        name="results",
    )(mixed, fresh)


def shards(
    hidden,
    queries,
    cache,
    cache_lengths,
    wkv,
    wo,
    attn_gain,
    moe_gain,
    w_gate,
    w_up,
    w_down,
    expert_ids,
    gates,
):
    x_wide, resid, fresh = prelude(
        hidden, queries, cache, cache_lengths, wkv, wo, attn_gain, moe_gain, expert_ids, gates
    )
    mixed = expert_layer(x_wide, resid, w_gate[0], w_up[0], w_down[0])
    mixed, fresh = results(mixed, fresh)
    fresh_key_value = fresh.reshape(hidden.shape[0], *wkv.shape[1:])
    return (mixed, fresh_key_value)


def solution(mesh):
    in_specs = (
        P(("grp", "tok"), "mdl"),
        P(("grp", "tok"), "mdl", None),
        P(("grp", "tok"), None, "mdl", None, None),
        P(("grp", "tok")),
        P("tok", "mdl", None, None),
        P("mdl", None, "tok"),
        P(),
        P(),
        P(("tok", "mdl"), None, None),
        P(("tok", "mdl"), None, None),
        P(("tok", "mdl"), None, None),
        P(("grp", "tok", "mdl"), None),
        P(("grp", "tok", "mdl"), None),
    )
    out_specs = (P(("grp", "tok", "mdl"), None), P(("grp", "tok"), "mdl", None, None))
    return jax.shard_map(shards, mesh=mesh, in_specs=in_specs, out_specs=out_specs, check_vma=False)
```
